256 devices in a mesh: seq: 128 (over z, x, y), head: 2 (over core).
Axes of the slice: x: 4, y: 4, z: 8, core: 2. Of those that a mesh axis runs over, the one named last changes fastest.
Arguments:
- queries: bfloat16 [32768, 32, 128], P('seq', 'head'), may hold values from -192 to 192
- keys: bfloat16 [32768, 8, 128], P(('seq', 'head')), may hold values from -6 to 6
- values: bfloat16 [32768, 8, 128], P(('seq', 'head')), may hold values from -6 to 6
- doc_start: int32 [32768], P('seq'), may hold values from 0 to 32767, as said below
- tile_list: int32 [128, 18], P('seq'), may hold values from 0 to 255, as said below
- tile_count: int32 [128], P('seq'), may hold values from 2 to 18, as said below
Outputs:
- attention_out: bfloat16 [32768, 32, 128], P('seq', 'head')
The draws below stay inside these ranges and needn't reach their ends.
Inputs may be any that keep to these rules, and one draw needn't show every extreme that they name: doc_start never falls, doc_start[i] <= i, and a new document begins at each position where it changes; documents hold 1 to 2048 tokens, one exactly 2048. `tile_list`: row s holds in its first tile_count[s] entries, ascending, exactly the tiles (tile t holds key positions t * 128 to t * 128 + 127) that contain a key visible to some query of positions s * 256 to s * 256 + 255; the later entries equal s * 2. `tile_count`: some row reaches 18.
All inputs are finite; a program needn't handle non-finite values.
Results may differ from the reference program's by a relative error of at most 0.004.
Values may be sent and summed in bfloat16 or wider, within the bound.
A program may use at most 64 MiB of HBM per device.

```python
import jax
import jax.numpy as jnp
from jax import lax

HQ = 32
KVH = 8
HD = 128
TOK_DEV = 256
TILE = 128
MAXDOC = 2048
REACH = 8
MAXT = 18
TOKENS = 32768
N_SEQ = 128


def document_starts(key):
    base_key = jax.random.fold_in(key, 11)
    choose_long = jax.random.randint(jax.random.fold_in(base_key, 1), (TOKENS,), 0, 2)
    short_len = jax.random.randint(jax.random.fold_in(base_key, 2), (TOKENS,), 1, TILE + 1)
    long_len = jax.random.randint(jax.random.fold_in(base_key, 3), (TOKENS,), TILE + 1, MAXDOC + 1)
    lengths = jnp.where(choose_long == 0, short_len, long_len).astype(jnp.int32)
    doc_ends = jnp.cumsum(lengths).astype(jnp.int32)
    start_marks = jnp.zeros((TOKENS,), jnp.int32).at[doc_ends].set(1, mode='drop')
    start_marks = start_marks.at[0].set(1)
    chosen = jax.random.randint(jax.random.fold_in(base_key, 4), (), REACH, N_SEQ).astype(jnp.int32)
    first_pos = chosen * TOK_DEV - MAXDOC + 1
    after_pos = chosen * TOK_DEV + 1
    position = jnp.arange(TOKENS, dtype=jnp.int32)
    inside = (position > first_pos) & (position < after_pos)
    start_marks = jnp.where(inside, 0, start_marks)
    start_marks = jnp.where((position == first_pos) | (position == after_pos), 1, start_marks)
    return lax.cummax(jnp.where(start_marks == 1, position, 0), axis=0).astype(jnp.int32)


def tile_tables(key):
    starts = document_starts(key)
    tiles_own = TOK_DEV // TILE
    first_tile = (starts[::TOK_DEV] // TILE).astype(jnp.int32)
    own_first = jnp.arange(N_SEQ, dtype=jnp.int32) * tiles_own
    slot_ids = jnp.arange(MAXT, dtype=jnp.int32)
    live_count = own_first + tiles_own - first_tile
    listed = first_tile[:, None] + slot_ids[None, :]
    listed = jnp.where(slot_ids[None, :] < live_count[:, None], listed, own_first[:, None])
    return (listed.astype(jnp.int32), live_count.astype(jnp.int32))


def attention_draws(key):
    base_key = jax.random.fold_in(key, 23)
    keys_raw = jax.random.truncated_normal(jax.random.fold_in(base_key, 1), -6.0, 6.0, (TOKENS, KVH, HD), jnp.float32)
    queries_raw = jax.random.truncated_normal(jax.random.fold_in(base_key, 2), -6.0, 6.0, (TOKENS, HQ, HD), jnp.float32)
    return (queries_raw, keys_raw)


def draw_queries(key, part):
    return attention_draws(key)[0].astype(jnp.bfloat16)


def draw_keys(key, part):
    return attention_draws(key)[1].astype(jnp.bfloat16)


def draw_doc_start(key, part):
    return document_starts(key)


def draw_tile_list(key, part):
    return tile_tables(key)[0]


def draw_tile_count(key, part):
    return tile_tables(key)[1]


def block_levels(rng, dims, cuts, low, high):
    level, own = 1.0, jax.random.fold_in(rng, 6)
    for dim, shards_of in cuts:
        draws = jnp.exp(jax.random.uniform(jax.random.fold_in(own, dim), (shards_of,), jnp.float32, low / len(cuts), high / len(cuts)))
        level = level * jnp.repeat(draws, dims[dim] // shards_of).reshape([-1 if axis == dim else 1 for axis in range(len(dims))])
    return level


def noise(own_key, shape, spread, reach, split=(), held_as=jnp.bfloat16):
    array = jax.random.normal(own_key, shape, jnp.float32) * spread
    if len(split) > 0:
        array = block_levels(own_key, shape, split, -0.22, 0.18) * array
    return jnp.clip(array, min=-reach, max=reach).astype(held_as)


def setup_inputs(seed: int = 0) -> dict:
    splits = jax.random.split(jax.random.key(seed), 7)
    queries = draw_queries(jax.random.fold_in(splits[6], 71), 0)
    keys = draw_keys(jax.random.fold_in(splits[6], 71), 0)
    values = noise(splits[2], (TOKENS, KVH, HD), 1.0, 6.0, ((0, 256),))
    doc_start = draw_doc_start(jax.random.fold_in(splits[6], 71), 0)
    tile_list = draw_tile_list(jax.random.fold_in(splits[6], 71), 0)
    tile_count = draw_tile_count(jax.random.fold_in(splits[6], 71), 0)
    return dict(queries=queries, keys=keys, values=values, doc_start=doc_start, tile_list=tile_list, tile_count=tile_count)


def reference(queries, keys, values, doc_start, tile_list, tile_count):
    group_size = HQ // KVH
    score_scale = 1.0 / (HD ** 0.5)
    key_tiles = keys.reshape(TOKENS // TILE, TILE, KVH, HD)
    value_tiles = values.reshape(TOKENS // TILE, TILE, KVH, HD)

    def one_shard(shard_index):
        query_block = lax.dynamic_slice_in_dim(queries, (shard_index * TOK_DEV).astype(jnp.int32), TOK_DEV, 0)
        starts = lax.dynamic_slice_in_dim(doc_start, (shard_index * TOK_DEV).astype(jnp.int32), TOK_DEV, 0)
        listed = tile_list[shard_index]
        live_count = tile_count[shard_index]
        key_block = key_tiles[listed].reshape(MAXT * TILE, KVH, HD)
        value_block = value_tiles[listed].reshape(MAXT * TILE, KVH, HD)
        key_pos = (listed[:, None] * TILE + jnp.arange(TILE, dtype=jnp.int32)[None, :]).reshape(-1)
        live_slot = jnp.repeat(jnp.arange(MAXT, dtype=jnp.int32) < live_count, TILE)
        query_pos = (shard_index * TOK_DEV).astype(jnp.int32) + jnp.arange(TOK_DEV, dtype=jnp.int32)
        visible = (key_pos[None, :] >= starts[:, None]) & (key_pos[None, :] <= query_pos[:, None]) & live_slot[None, :]
        grouped = query_block.reshape(TOK_DEV, KVH, group_size, HD).astype(jnp.float32)
        scores = jnp.einsum("tgch,kgh->gctk", grouped, key_block.astype(jnp.float32)) * score_scale
        scores = jnp.where(visible[None, None], scores, -jnp.inf)
        row_top = jnp.max(scores, axis=-1, keepdims=True)
        weights = jnp.where(visible[None, None], jnp.exp(scores - row_top), jnp.float32(0.0))
        weight_sum = jnp.sum(weights, axis=-1)
        rounded = lax.optimization_barrier(weights.astype(jnp.bfloat16)).astype(jnp.float32)
        summed = jnp.einsum("gctk,kgh->gcth", rounded, value_block.astype(jnp.float32))
        result = summed / weight_sum[..., None]
        result = jnp.transpose(result, (2, 0, 1, 3)).reshape(TOK_DEV, HQ, HD)
        return result.astype(jnp.bfloat16)

    blocks = lax.map(one_shard, jnp.arange(N_SEQ, dtype=jnp.int32))
    return blocks.reshape(TOKENS, HQ, HD)
```

```python
import jax
import jax.numpy as jnp
from jax import lax
from jax.experimental import pallas as pl
from jax.experimental.pallas import tpu as pltpu
from jax.sharding import PartitionSpec as P

TILE = 128
REACH = 8
BACK = REACH + 1
SIDE = 4
HEADS = 4
GROUP = 4
TOK = 256
HD = 128
ENTRIES = BACK * HEADS
FIRST = 2
NEG = -1e30
FAR = 1 << 20
MESH = pl.DeviceIdType.MESH

PLAN = (
    (54547458, 326392868, 309400822, 553747682, 503431366, 274251856, 339108337, 151355832, 184951328, 495388016, 537034880, 218448288),
    (5279796, 309644368, 271925456, 394514453, 205652514, 289884273, 169332072, 471957680, 155732196, 505987401, 67502496, 537313680),
    (4247573, 37815575, 134603059, 276144324, 556163184, 253855040, 151082279, 189202642, 587637248, 570655202, 352831649, 453460352),
    (54562820, 207699988, 497325315, 134536528, 394780880, 471096760, 505659720, 436767856, 590512304, 378601856, 537022995, 235290720),
)


def attend(queries_t, window, thresholds, top, total, summed, back, head, own):
    scale = HD ** (-0.5) * 1.4426950408889634
    key_tile = window[back, head, 0]
    value_tile = window[back, head, 1]
    iota = lax.broadcasted_iota(jnp.int32, (TILE, TOK), 0)
    for member in range(GROUP):
        span = slice(member * TOK, (member + 1) * TOK)
        scores = jnp.dot(
            key_tile, queries_t[head, :, span], preferred_element_type=jnp.float32
        )
        halves = []
        for half in range(2):
            low = thresholds[pl.ds(back * 2 + half, 1), :]
            seen = iota >= low
            if own:
                seen = seen & (
                    iota + half * TILE <= lax.broadcasted_iota(jnp.int32, (TILE, TOK), 1)
                )
            halves.append(jnp.where(seen, scores[half * TILE : (half + 1) * TILE], NEG))
        scores = jnp.concatenate(halves, axis=0)
        new_top = jnp.max(scores, axis=0, keepdims=True)
        if not own:
            old_top = top[head, :, span]
            new_top = jnp.maximum(old_top, new_top)
        scaled_top = new_top * scale
        weights = jnp.exp2(scores * scale - scaled_top)
        weight_sum = jnp.sum(weights, axis=0, keepdims=True)
        product = lax.dot_general(
            value_tile,
            weights.astype(jnp.bfloat16),
            (((0,), (0,)), ((), ())),
            preferred_element_type=jnp.float32,
        )
        if not own:
            factor = jnp.exp2(old_top * scale - scaled_top)
            weight_sum = total[head, :, span] * factor + weight_sum
            product = summed[head, :, span] * factor + product
        top[head, :, span] = new_top
        total[head, :, span] = weight_sum
        summed[head, :, span] = product


def kernel(
    q_ref,
    k_ref,
    v_ref,
    start_ref,
    list_ref,
    count_ref,
    o_ref,
    window,
    queries_t,
    thresholds,
    top,
    total,
    summed,
    result,
    local_sem,
    swap_send,
    swap_recv,
    send_sem,
    recv_sem,
):
    seq = lax.axis_index("seq")
    core = lax.axis_index("head")
    devices = lax.axis_size("seq")
    place = lax.rem(seq, SIDE)
    row_first = seq - place
    neighbours = (
        row_first + lax.rem(place + 1, SIDE),
        row_first + lax.rem(place + SIDE - 1, SIDE),
        lax.rem(seq + SIDE, devices),
        lax.rem(seq + devices - SIDE, devices),
    )
    last = place == SIDE - 1
    none = place == 0
    shifts = (
        jnp.where(last, 1 - SIDE, 1),
        jnp.where(none, SIDE - 1, -1),
        SIDE,
        -SIDE,
    )

    barrier = pltpu.get_barrier_semaphore()
    for where in neighbours:
        pl.semaphore_signal(
            barrier, inc=1, device_id=(where, core), device_id_type=MESH
        )
    pl.semaphore_signal(barrier, inc=1, device_id=(seq, 1 - core), device_id_type=MESH)

    locals_ = []
    for part, ref in enumerate((k_ref, v_ref)):
        locals_.append(
            pltpu.make_async_copy(
                ref.at[pl.ds(core * HEADS, HEADS)],
                window.at[0, :, part, pl.ds(core * TILE, TILE), :],
                local_sem.at[part],
            )
        )
    for copy in locals_:
        copy.start()
    pl.semaphore_wait(barrier, 5)
    swaps = []
    for part, ref in enumerate((k_ref, v_ref)):
        swaps.append(
            pltpu.make_async_remote_copy(
                src_ref=ref.at[pl.ds((1 - core) * HEADS, HEADS)],
                dst_ref=window.at[0, :, part, pl.ds(core * TILE, TILE), :],
                send_sem=swap_send.at[part],
                recv_sem=swap_recv.at[part],
                device_id=(seq, 1 - core),
                device_id_type=MESH,
            )
        )
    for copy in swaps:
        copy.start()

    tile_row = lax.broadcasted_iota(jnp.int32, (24, 1), 0)
    back_of = tile_row // 2
    half_of = tile_row - 2 * back_of
    tile_id = 2 * (seq - back_of) + half_of
    slots = list_ref.shape[1]
    listed = (list_ref[...] == tile_id) & (
        lax.broadcasted_iota(jnp.int32, (1, slots), 1) < count_ref[0]
    )
    live = jnp.max(jnp.where(listed, 1.0, 0.0), axis=1, keepdims=True)
    low = start_ref[...] - seq * TOK + (back_of * TOK - half_of * TILE)
    thresholds[...] = jnp.where(live > 0.5, low, FAR)

    for head in range(HEADS):
        for member in range(GROUP):
            queries_t[head, :, member * TOK : (member + 1) * TOK] = q_ref[
                :, head * GROUP + member, :
            ].T

    def hand_on(slot, part, direction):
        back, head = slot // HEADS, lax.rem(slot, HEADS)
        there = back + shifts[direction]
        return pltpu.make_async_remote_copy(
            src_ref=window.at[back, head, part],
            dst_ref=window.at[there, head, part],
            send_sem=send_sem.at[slot, part, direction],
            recv_sem=recv_sem.at[there * HEADS + head, part],
            device_id=(neighbours[direction], core),
            device_id_type=MESH,
        )

    def arrived(slot, part):
        back, head = slot // HEADS, lax.rem(slot, HEADS)
        return pltpu.make_async_remote_copy(
            src_ref=window.at[back, head, part],
            dst_ref=window.at[back, head, part],
            send_sem=send_sem.at[slot, part, 0],
            recv_sem=recv_sem.at[slot, part],
            device_id=(neighbours[0], core),
            device_id_type=MESH,
        )

    words = []
    for j in range(ENTRIES // 3):
        word = PLAN[0][j]
        for c in range(1, SIDE):
            word = jnp.where(place == c, PLAN[c][j], word)
        words.append(word)

    def entry(n):
        j, third = n // 3, lax.rem(n, 3)
        word = words[0]
        for i in range(1, ENTRIES // 3):
            word = jnp.where(j == i, words[i], word)
        divisor = jnp.where(third == 0, 1, jnp.where(third == 1, 1024, 1048576))
        code = lax.rem(word // divisor, 1024)
        return code // 16, lax.rem(code, 16)

    def relay(slot, directions):
        for part in range(2):

            @pl.when(slot >= HEADS)
            def _():
                arrived(slot, part).wait_recv()

            for direction in range(4):

                @pl.when(lax.rem(directions // (1 << direction), 2) == 1)
                def _():
                    hand_on(slot, part, direction).start()

    for copy in locals_:
        copy.wait()
    for copy in swaps:
        copy.wait()

    for n in range(FIRST):
        relay(*entry(n))
    for head in range(HEADS):
        attend(queries_t, window, thresholds, top, total, summed, 0, head, True)

    def step(n, _):
        slot, directions = entry(n)
        relay(slot, directions)

        @pl.when(slot >= HEADS)
        def _():
            back, head = slot // HEADS, lax.rem(slot, HEADS)
            attend(queries_t, window, thresholds, top, total, summed, back, head, False)

        return 0

    lax.fori_loop(FIRST, ENTRIES, step, 0)

    for head in range(HEADS):
        for member in range(GROUP):
            span = slice(member * TOK, (member + 1) * TOK)
            inverse = 1.0 / total[head, :, span]
            result[:, head * GROUP + member, :] = (summed[head, :, span] * inverse).T
    o_ref[...] = result[...].astype(jnp.bfloat16)

    def finish(n, _):
        slot, directions = entry(n)
        for part in range(2):
            for direction in range(4):

                @pl.when(lax.rem(directions // (1 << direction), 2) == 1)
                def _():
                    hand_on(slot, part, direction).wait_send()

        return 0

    lax.fori_loop(0, ENTRIES, finish, 0)


def body(queries, keys, values, doc_start, tile_list, tile_count):
    keys_t = jnp.swapaxes(keys, 0, 1)
    values_t = jnp.swapaxes(values, 0, 1)
    vmem = pl.BlockSpec(memory_space=pltpu.VMEM)
    hbm = pl.BlockSpec(memory_space=pltpu.HBM)
    lanes = GROUP * TOK
    return pl.pallas_call(
        kernel,
        out_shape=jax.ShapeDtypeStruct(queries.shape, jnp.bfloat16),
        in_specs=[vmem, hbm, hbm, vmem, vmem, pl.BlockSpec(memory_space=pltpu.SMEM)],
        out_specs=vmem,
        scratch_shapes=[
            pltpu.VMEM((BACK, HEADS, 2, TOK, HD), jnp.bfloat16),
            pltpu.VMEM((HEADS, HD, lanes), jnp.bfloat16),
            pltpu.VMEM((24, TOK), jnp.int32),
            pltpu.VMEM((HEADS, 1, lanes), jnp.float32),
            pltpu.VMEM((HEADS, 1, lanes), jnp.float32),
            pltpu.VMEM((HEADS, HD, lanes), jnp.float32),
            pltpu.VMEM(queries.shape, jnp.float32),
            pltpu.SemaphoreType.DMA((2,)),
            pltpu.SemaphoreType.DMA((2,)),
            pltpu.SemaphoreType.DMA((2,)),
            pltpu.SemaphoreType.DMA((ENTRIES, 2, 4)),
            pltpu.SemaphoreType.DMA((ENTRIES, 2)),
        ],
        compiler_params=pltpu.CompilerParams(collective_id=0, has_side_effects=True),
    )(queries, keys_t, values_t, doc_start.reshape(1, TOK), tile_list, tile_count)


def solution(mesh):
    in_specs = (
        P("seq", "head", None),
        P(("seq", "head"), None, None),
        P(("seq", "head"), None, None),
        P("seq"),
        P("seq", None),
        P("seq"),
    )
    return jax.shard_map(
        body, mesh=mesh, in_specs=in_specs, out_specs=P("seq", "head", None), check_vma=False
    )
```

```python
import jax
import jax.numpy as jnp
from jax import lax
from jax.experimental import pallas as pl
from jax.experimental.pallas import tpu as pltpu
from jax.sharding import PartitionSpec as P

TILE = 128
REACH = 8
BACK = REACH + 1
SIDE = 4
HEADS = 4
GROUP = 4
TOK = 256
HD = 128
ENTRIES = BACK * HEADS
FIRST = 2
TURN = 5
NEG = -1e30
FAR = 1 << 20
MESH = pl.DeviceIdType.MESH

PLAN = (
    (133376, 134400, 137664, 138688, 131264, 132288, 166336, 167377, 135360, 136384, 170368, 162048, 143680, 171411, 163087, 144704, 198662, 157952, 145472, 199713, 158989, 202752, 146503, 160128, 194624, 139264, 151680, 176256, 140292, 161152, 203790, 141411, 152704, 195658, 142431, 177280, 180741, 178176, 190528, 181782, 179224, 147456, 191552, 149527, 153885, 192576, 188928, 172032, 193600, 148480, 189982, 164168, 150556, 186368, 154889, 155648, 168203, 173076, 184320, 156672, 196608, 165196, 182288, 187392, 174107, 169234, 175104, 200725, 183321, 197632, 185376, 26, 201762, 0, 0, 0, 0, 0, 0, 0),
    (137536, 138560, 133440, 134464, 135424, 136448, 170112, 131392, 132416, 171155, 145408, 166080, 146439, 155904, 167121, 139328, 156940, 168128, 140356, 159872, 169170, 174592, 160910, 164096, 175637, 161792, 165136, 143616, 162831, 141376, 188608, 144646, 142400, 189632, 158080, 151557, 28, 196736, 147712, 152586, 197760, 159136, 153869, 176320, 192640, 154891, 190592, 148744, 202752, 177344, 184342, 149824, 191616, 193693, 203806, 180224, 185344, 150883, 26, 186432, 194560, 198665, 181248, 178200, 199713, 187456, 195584, 200731, 31, 182272, 179200, 201751, 34, 183296, 172057, 173076, 0, 0, 0, 0),
    (131392, 132416, 135488, 136512, 137472, 138496, 145472, 164032, 146503, 133440, 134464, 165072, 141312, 168320, 142341, 160000, 169362, 139584, 161038, 170432, 140612, 161792, 171475, 174144, 162831, 166336, 175189, 155776, 167377, 147456, 200832, 176128, 156812, 192640, 148488, 182272, 201890, 177152, 183318, 193689, 149504, 151582, 202880, 196608, 152586, 172032, 150537, 187008, 203939, 197632, 188448, 173076, 184320, 188059, 198656, 180224, 153600, 185370, 199680, 178209, 157952, 154635, 189468, 158976, 181261, 24, 194560, 143360, 190464, 179223, 195615, 144390, 191517, 0, 0, 0, 0, 0, 0, 0),
    (135424, 136448, 137472, 138496, 139264, 168128, 140292, 131328, 132352, 133376, 134400, 169170, 143360, 161792, 170432, 144390, 162831, 171456, 153875, 155904, 172032, 164288, 156940, 154891, 165312, 191120, 141312, 166208, 192157, 142341, 167232, 160145, 173056, 157696, 202836, 161166, 147712, 203840, 158720, 194723, 178765, 196800, 195743, 148736, 188616, 184832, 145408, 179799, 186496, 176128, 182784, 197856, 200704, 146439, 174080, 189632, 185884, 151680, 183834, 198720, 177177, 175104, 187542, 201749, 149504, 199771, 34, 152704, 192545, 150538, 193545, 180254, 181272, 0, 0, 0, 0, 0, 0, 0),
    (133376, 134400, 137664, 138688, 131264, 132288, 166336, 167377, 135360, 136384, 170368, 162048, 143680, 171411, 163087, 144704, 198662, 157952, 199713, 145472, 158989, 202752, 146503, 160128, 194624, 139264, 151680, 176256, 140292, 161152, 203790, 141411, 152704, 195658, 142400, 180767, 177285, 178176, 149504, 190550, 179223, 181760, 191576, 153856, 147456, 150528, 192605, 164169, 188928, 193630, 154891, 189952, 148508, 172032, 184328, 186368, 165200, 155648, 168192, 173076, 156672, 169216, 196620, 174098, 182272, 187419, 175104, 185365, 200730, 183321, 197664, 201762, 0, 0, 0, 0, 0, 0, 0, 0),
    (137536, 138560, 133440, 134464, 170112, 135424, 136448, 171155, 131392, 132416, 145408, 166080, 155904, 146432, 167111, 156945, 139328, 168140, 159872, 140352, 169156, 18, 160896, 174592, 164110, 161792, 175616, 165141, 16, 162816, 143616, 188623, 158080, 141376, 144640, 189638, 28, 159104, 142400, 151552, 196749, 147717, 152576, 197770, 192640, 153856, 176352, 148744, 154880, 177355, 184342, 202752, 190592, 193694, 149824, 180224, 185370, 203776, 191651, 194589, 150848, 186441, 178176, 198656, 187483, 195615, 199680, 181281, 179224, 200704, 182295, 172032, 183321, 201762, 173076, 0, 0, 0, 0, 0),
    (131392, 132416, 135488, 136512, 137472, 138496, 164032, 145472, 165056, 146512, 133440, 134471, 168320, 141312, 160000, 169362, 142341, 161024, 170446, 139584, 171456, 161811, 140612, 166336, 162816, 174159, 167377, 175168, 155797, 200832, 147456, 156812, 192640, 176128, 182272, 201890, 148480, 183304, 172057, 177152, 151574, 193664, 196638, 152586, 202880, 149504, 178176, 173076, 197632, 187040, 203939, 150528, 180233, 198656, 184320, 188059, 199713, 185344, 153600, 188442, 157952, 181272, 154635, 179223, 158989, 189468, 194560, 143360, 190464, 195615, 144390, 191517, 0, 0, 0, 0, 0, 0, 0, 0),
    (135424, 136448, 137472, 138496, 139264, 168128, 140288, 169156, 131328, 132352, 133376, 134418, 143360, 170432, 161792, 144390, 171456, 162835, 172047, 164288, 155904, 153856, 165328, 156940, 173056, 166208, 191124, 154891, 167232, 192145, 141341, 202816, 160128, 142341, 157696, 203840, 161187, 178752, 186496, 158720, 194702, 13, 147712, 188608, 195743, 179799, 196800, 184832, 145408, 148744, 189632, 176156, 174080, 187547, 200704, 146439, 182784, 197824, 185888, 151680, 175130, 198720, 177173, 183808, 199766, 201728, 149529, 192545, 152738, 193546, 150558, 180233, 181272, 0, 0, 0, 0, 0, 0, 0),
    (133376, 134400, 137664, 138688, 131264, 132288, 166336, 167377, 135360, 136384, 170368, 162048, 143680, 171411, 163087, 144704, 198662, 157952, 199713, 145472, 158989, 202752, 146503, 160128, 194624, 139264, 151680, 176256, 140292, 161152, 203790, 141411, 152704, 195658, 142400, 180767, 177285, 178176, 149504, 190550, 179223, 181760, 191576, 147456, 153856, 150528, 192605, 9, 172032, 188928, 193630, 164160, 189952, 148508, 8, 186368, 154880, 184331, 196608, 173056, 155668, 168192, 187419, 165184, 156672, 182288, 174092, 169216, 197650, 175104, 185376, 200725, 183322, 201753, 34, 0, 0, 0, 0, 0),
    (137536, 138560, 133440, 134464, 170112, 135424, 136448, 171155, 131392, 132416, 145408, 166080, 155904, 146432, 167111, 156945, 139328, 168140, 159872, 140352, 169156, 18, 160896, 174592, 164110, 161792, 175616, 165141, 16, 162816, 143616, 188623, 158080, 141376, 144640, 189638, 28, 159104, 142400, 151552, 196749, 147717, 152576, 197770, 192640, 153856, 176352, 148744, 154880, 190603, 184320, 202752, 177366, 193694, 149824, 191645, 185370, 203776, 180259, 194560, 150848, 186441, 195615, 198656, 181272, 178176, 199680, 187489, 27, 179200, 200704, 182295, 201728, 183330, 25, 172032, 173076, 0, 0, 0),
    (131392, 132416, 135488, 136512, 137472, 138496, 164032, 145472, 165056, 146512, 133440, 134471, 168320, 141312, 160000, 169362, 142341, 161024, 170446, 139584, 171456, 161811, 140612, 166336, 162816, 174159, 167377, 175168, 155797, 200832, 147456, 156812, 192640, 176128, 182272, 201890, 148480, 183304, 193689, 177152, 151582, 202880, 196630, 152586, 172032, 149504, 188416, 203939, 197632, 187040, 173076, 150528, 180233, 198656, 184320, 188059, 199713, 185344, 153600, 178202, 157952, 189468, 154635, 181272, 158989, 143360, 190464, 194560, 179223, 195615, 144390, 191517, 0, 0, 0, 0, 0, 0, 0, 0),
    (135424, 136448, 137472, 138496, 139264, 168128, 140288, 169156, 131328, 132352, 133376, 134418, 143360, 170432, 161792, 144390, 171456, 162835, 172047, 164288, 155904, 153856, 165328, 156940, 173056, 166208, 191124, 154891, 167232, 192145, 141341, 202816, 160128, 142341, 157696, 203840, 161187, 178766, 196800, 158720, 194701, 147712, 188608, 195743, 179799, 186496, 184832, 145408, 148744, 197824, 176160, 174080, 189660, 200704, 146432, 182791, 198720, 185882, 151680, 175104, 187541, 177179, 183808, 199744, 201750, 149529, 192545, 152738, 193546, 150528, 180254, 9, 181272, 0, 0, 0, 0, 0, 0, 0),
    (133376, 134400, 137664, 138688, 131264, 132288, 166336, 167377, 135360, 136384, 170368, 162048, 143680, 171411, 163087, 144704, 198662, 157952, 199713, 145472, 158989, 202752, 146503, 160128, 194624, 139264, 151680, 176256, 140292, 161152, 203790, 141411, 152704, 195658, 142400, 180767, 177285, 178176, 149504, 190550, 179223, 181760, 191576, 153856, 150557, 192585, 172032, 188928, 193630, 164160, 147456, 189980, 186368, 154891, 148480, 184328, 173076, 168192, 196608, 165200, 155648, 182272, 174080, 187419, 156672, 169228, 175104, 185344, 200722, 21, 183296, 197658, 25, 201760, 34, 0, 0, 0, 0, 0),
    (137536, 138560, 133440, 134464, 170112, 135424, 136448, 171155, 131392, 132416, 145408, 166080, 155904, 146432, 167111, 156945, 139328, 168140, 159872, 140352, 169156, 18, 160896, 174592, 164110, 161792, 175616, 165141, 16, 162816, 143616, 188623, 158080, 144640, 189638, 28, 159104, 141376, 151552, 196749, 147712, 142400, 152576, 197765, 10, 192640, 153856, 176352, 148744, 154880, 190603, 184320, 202752, 177366, 193694, 149824, 191645, 185370, 203776, 180259, 194560, 150848, 186441, 195615, 198656, 181272, 178176, 199680, 187489, 27, 179200, 200704, 182295, 201728, 183330, 25, 172032, 173076, 0, 0),
    (131392, 132416, 135488, 136512, 137472, 138496, 164032, 145472, 165056, 146512, 133440, 134471, 168320, 141312, 160000, 169362, 142341, 161024, 170446, 139584, 171456, 161811, 140612, 166336, 162816, 174159, 167377, 175168, 155797, 200832, 147456, 156812, 192640, 176128, 182272, 201890, 148480, 183304, 193689, 177152, 151582, 202880, 196630, 152586, 172032, 197632, 188448, 203939, 149504, 187008, 173076, 150528, 180233, 198656, 184320, 188059, 199713, 185344, 178202, 153600, 157952, 189468, 181272, 158989, 154624, 179211, 190464, 194583, 143360, 195615, 144390, 191517, 0, 0, 0, 0, 0, 0, 0, 0),
    (135424, 136448, 137472, 138496, 139264, 168128, 140288, 169156, 131328, 132352, 133376, 134418, 143360, 170432, 161792, 144390, 171456, 162835, 172047, 164288, 155904, 153856, 165328, 156940, 173056, 166208, 191124, 154891, 167232, 192145, 141341, 202816, 160128, 142341, 203840, 161187, 178752, 157710, 196800, 194688, 147712, 158733, 188608, 195743, 179776, 186496, 184855, 148744, 197824, 176160, 174080, 189660, 200704, 145408, 182784, 198720, 185882, 175125, 187520, 177152, 151707, 183830, 199744, 201728, 146457, 192512, 149537, 34, 193536, 152711, 30, 180224, 150538, 9, 181272, 0, 0, 0, 0, 0),
    (131328, 132352, 137344, 138368, 135488, 136512, 166336, 167377, 170368, 133568, 134592, 162048, 143680, 171411, 163087, 144704, 198662, 157952, 199680, 145505, 158989, 202752, 146503, 160128, 194624, 139264, 151680, 176256, 140292, 161152, 203790, 141411, 152704, 195658, 142400, 180767, 177285, 178176, 149504, 190550, 179223, 181760, 191576, 172032, 150557, 192585, 164160, 188928, 193630, 153856, 147456, 184320, 154891, 186368, 189952, 148508, 173056, 196616, 168212, 165184, 187392, 155648, 182288, 174107, 169234, 197632, 175136, 185344, 200725, 156672, 183322, 201740, 25, 34, 0, 0, 0, 0, 0, 0),
    (131392, 132416, 137472, 138496, 135424, 136448, 170112, 171155, 133440, 134464, 166080, 143424, 155904, 167121, 144454, 156928, 168128, 174604, 159872, 169170, 175637, 160896, 164096, 141582, 161792, 165136, 142597, 162816, 188608, 151567, 158080, 189660, 152586, 159104, 196736, 153869, 192640, 197760, 154912, 11, 147712, 176320, 202752, 184320, 190592, 149824, 178176, 177344, 203798, 35, 193664, 191616, 150878, 29, 148736, 180224, 198656, 145417, 185344, 186432, 199688, 146458, 139264, 181248, 200737, 7, 179200, 187456, 172056, 194560, 182272, 201751, 27, 195584, 183330, 173087, 140313, 20, 4, 0),
    (135424, 136448, 131392, 132416, 137536, 138560, 133440, 134464, 164032, 139328, 165056, 140368, 4, 168320, 160000, 169362, 161038, 170432, 141312, 161792, 171475, 142341, 182272, 166336, 174144, 162831, 167377, 151872, 183296, 200857, 175189, 155776, 192640, 152906, 187008, 201890, 176128, 156812, 193664, 147678, 177152, 188032, 202902, 196635, 172032, 143360, 188416, 197664, 203939, 180224, 184320, 144384, 173062, 178196, 157952, 198656, 148672, 189448, 28, 185344, 199680, 145690, 159009, 181261, 149528, 146695, 194560, 150528, 179209, 23, 153600, 190464, 195584, 154655, 11, 191517, 0, 0, 0, 0),
    (133376, 134400, 135424, 136448, 168128, 131328, 132352, 162048, 169170, 163087, 137472, 138496, 170432, 139264, 191104, 171456, 140307, 4, 192128, 145664, 164317, 194688, 146695, 165328, 157696, 141312, 166208, 158733, 142336, 167237, 195712, 172032, 202833, 31, 147456, 203875, 184832, 173076, 196800, 143360, 176128, 148488, 188608, 200704, 178752, 186496, 144384, 185862, 179776, 197850, 153728, 177152, 174103, 189664, 154752, 201728, 182784, 198742, 151580, 175104, 187531, 160034, 199744, 152597, 183808, 192539, 33, 161024, 193546, 25, 155648, 180224, 149518, 156702, 181248, 150540, 24, 9, 0, 0),
    (131200, 132224, 135360, 136384, 163904, 137408, 138432, 164944, 133248, 134272, 168000, 155776, 141376, 169042, 156812, 142400, 198661, 161920, 199680, 143457, 162959, 202752, 144454, 159872, 165888, 139264, 147584, 166929, 140292, 160896, 194638, 170048, 148616, 176256, 171091, 157824, 203811, 151552, 158861, 195648, 145439, 180736, 177302, 146439, 181760, 190552, 152576, 149514, 191552, 178205, 188928, 192576, 179223, 150537, 193600, 153694, 184320, 196608, 172032, 189980, 186368, 154699, 185370, 187392, 173083, 182272, 200724, 174080, 183321, 197632, 175136, 21, 201762, 0, 0, 0, 0, 0, 0, 0),
    (137280, 138304, 135232, 136256, 131136, 132160, 163968, 143360, 133184, 134208, 165008, 144390, 170112, 172096, 159744, 171155, 145472, 160782, 168128, 146503, 155776, 169170, 173120, 156820, 166028, 176128, 139264, 167057, 149504, 188608, 177152, 140310, 189636, 150528, 157852, 196745, 151552, 158861, 174144, 152576, 192650, 197792, 202752, 184320, 175189, 178752, 193694, 190592, 179776, 147479, 191645, 203776, 185379, 186458, 148488, 198656, 187483, 194560, 180224, 199713, 141312, 182272, 200704, 195615, 183296, 201753, 142370, 181248, 161797, 153624, 162831, 154635, 0, 0, 0, 0, 0, 0, 0, 0),
    (133184, 134208, 131136, 132160, 135232, 136256, 137280, 138304, 168128, 145472, 169152, 146514, 7, 163968, 143424, 157696, 164992, 144464, 6, 147584, 169984, 139328, 158733, 171008, 140371, 148612, 166080, 141384, 159744, 167104, 142417, 5, 151552, 200832, 180800, 160782, 192640, 153600, 152586, 201856, 176674, 155776, 193664, 154654, 11, 156800, 202880, 177676, 22, 149632, 203904, 181859, 150680, 198656, 196617, 161920, 199680, 197665, 32, 172032, 184320, 182848, 162959, 185344, 183898, 173081, 186900, 190464, 188416, 187931, 189468, 194560, 178176, 174080, 195615, 191517, 175125, 179223, 0, 0),
    (135168, 136192, 133120, 134144, 166080, 141312, 155776, 131072, 132096, 167104, 142353, 156800, 137216, 138245, 139264, 168128, 159884, 140292, 169152, 160914, 143360, 164046, 161792, 144390, 165056, 162832, 145408, 194639, 157824, 146439, 195648, 158879, 176704, 170189, 180352, 153600, 171219, 181400, 177728, 202816, 186902, 154635, 203840, 187939, 151552, 178267, 184832, 152586, 196800, 172032, 147456, 179287, 185882, 148480, 197824, 173064, 32, 174080, 198720, 200724, 149504, 199777, 182912, 175125, 183961, 150537, 201762, 192512, 188416, 189468, 190464, 193566, 191517, 0, 0, 0, 0, 0, 0, 0),
)


def attend(queries_t, window, thresholds, top, total, summed, back, head, own):
    scale = HD ** (-0.5) * 1.4426950408889634
    key_tile = window[back, head, 0]
    value_tile = window[back, head, 1]
    iota = lax.broadcasted_iota(jnp.int32, (TILE, TOK), 0)
    seen = []
    for half in range(2):
        mask = iota >= thresholds[pl.ds(back * 2 + half, 1), :]
        if own:
            mask = mask & (iota + half * TILE <= lax.broadcasted_iota(jnp.int32, (TILE, TOK), 1))
        seen.append(mask)
    spans = [slice(member * TOK, (member + 1) * TOK) for member in range(GROUP)]
    if not own:
        old_tops = [top[head, :, span] for span in spans]
        old_totals = [total[head, :, span] for span in spans]
    raw = [
        jnp.dot(key_tile, queries_t[head, :, span], preferred_element_type=jnp.float32)
        for span in spans
    ]
    tops, totals, factors, products = [], [], [], []
    for member in range(GROUP):
        scores = jnp.concatenate(
            [
                jnp.where(seen[half], raw[member][half * TILE : (half + 1) * TILE], NEG)
                for half in range(2)
            ],
            axis=0,
        )
        new_top = jnp.max(scores, axis=0, keepdims=True)
        if not own:
            new_top = jnp.maximum(old_tops[member], new_top)
        scaled_top = new_top * scale
        weights = jnp.exp2(scores * scale - scaled_top)
        weight_sum = jnp.sum(weights, axis=0, keepdims=True)
        products.append(
            lax.dot_general(
                value_tile,
                weights.astype(jnp.bfloat16),
                (((0,), (0,)), ((), ())),
                preferred_element_type=jnp.float32,
            )
        )
        if not own:
            factors.append(jnp.exp2(old_tops[member] * scale - scaled_top))
            weight_sum = old_totals[member] * factors[member] + weight_sum
        tops.append(new_top)
        totals.append(weight_sum)
    for member, span in enumerate(spans):
        top[head, :, span] = tops[member]
        total[head, :, span] = totals[member]
        if own:
            summed[head, :, span] = products[member]
        else:
            summed[head, :, span] = summed[head, :, span] * factors[member] + products[member]


def kernel(
    q_ref,
    k_ref,
    v_ref,
    start_ref,
    list_ref,
    count_ref,
    o_ref,
    window,
    queries_t,
    thresholds,
    top,
    total,
    summed,
    result,
    local_sem,
    swap_send,
    swap_recv,
    send_sem,
    recv_sem,
):
    seq = lax.axis_index("seq")
    core = lax.axis_index("head")
    devices = lax.axis_size("seq")
    place = lax.rem(seq, SIDE)
    row_first = seq - place
    neighbours = (
        row_first + lax.rem(place + 1, SIDE),
        row_first + lax.rem(place + SIDE - 1, SIDE),
        lax.rem(seq + SIDE, devices),
        lax.rem(seq + devices - SIDE, devices),
    )
    last = place == SIDE - 1
    none = place == 0
    shifts = (
        jnp.where(last, 1 - SIDE, 1),
        jnp.where(none, SIDE - 1, -1),
        SIDE,
        -SIDE,
    )

    row = seq // SIDE
    rows = devices // SIDE
    not_last = row < rows - 1
    not_first = row > 0

    barrier = pltpu.get_barrier_semaphore()
    for where, there in zip(neighbours, (None, None, not_last, not_first)):

        def greet(where=where):
            pl.semaphore_signal(barrier, inc=1, device_id=(where, core), device_id_type=MESH)

        if there is None:
            greet()
        else:
            pl.when(there)(greet)
    pl.semaphore_signal(barrier, inc=1, device_id=(seq, 1 - core), device_id_type=MESH)

    locals_ = []
    for part, ref in enumerate((k_ref, v_ref)):
        locals_.append(
            pltpu.make_async_copy(
                ref.at[pl.ds(core * HEADS, HEADS)],
                window.at[0, :, part, pl.ds(core * TILE, TILE), :],
                local_sem.at[part],
            )
        )
    for copy in locals_:
        copy.start()
    pl.semaphore_wait(
        barrier, 3 + jnp.where(not_last, 1, 0) + jnp.where(not_first, 1, 0)
    )
    swaps = []
    for part, ref in enumerate((k_ref, v_ref)):
        swaps.append(
            pltpu.make_async_remote_copy(
                src_ref=ref.at[pl.ds((1 - core) * HEADS, HEADS)],
                dst_ref=window.at[0, :, part, pl.ds(core * TILE, TILE), :],
                send_sem=swap_send.at[part],
                recv_sem=swap_recv.at[part],
                device_id=(seq, 1 - core),
                device_id_type=MESH,
            )
        )
    for copy in swaps:
        copy.start()

    tile_row = lax.broadcasted_iota(jnp.int32, (24, 1), 0)
    back_of = tile_row // 2
    half_of = tile_row - 2 * back_of
    tile_id = 2 * (seq - back_of) + half_of
    slots = list_ref.shape[1]
    listed = (list_ref[...] == tile_id) & (
        lax.broadcasted_iota(jnp.int32, (1, slots), 1) < count_ref[0]
    )
    live = jnp.max(jnp.where(listed, 1.0, 0.0), axis=1, keepdims=True)
    low = start_ref[...] - seq * TOK + (back_of * TOK - half_of * TILE)
    thresholds[...] = jnp.where(live > 0.5, low, FAR)

    for head in range(HEADS):
        for member in range(GROUP):
            queries_t[head, :, member * TOK : (member + 1) * TOK] = q_ref[
                :, head * GROUP + member, :
            ].T

    def hand_on(slot, part, direction):
        back, head = slot // HEADS, lax.rem(slot, HEADS)
        there = back + shifts[direction]
        return pltpu.make_async_remote_copy(
            src_ref=window.at[back, head, part],
            dst_ref=window.at[there, head, part],
            send_sem=send_sem.at[slot, part, direction],
            recv_sem=recv_sem.at[there * HEADS + head, part],
            device_id=(neighbours[direction], core),
            device_id_type=MESH,
        )

    def arrived(slot, part):
        back, head = slot // HEADS, lax.rem(slot, HEADS)
        return pltpu.make_async_remote_copy(
            src_ref=window.at[back, head, part],
            dst_ref=window.at[back, head, part],
            send_sem=send_sem.at[slot, part, 0],
            recv_sem=recv_sem.at[slot, part],
            device_id=(neighbours[0], core),
            device_id_type=MESH,
        )

    kind = jnp.where(
        row == rows - 1,
        5 * SIDE,
        jnp.where(row == rows - 2, 4 * SIDE, lax.rem(row, SIDE) * SIDE),
    )
    kind = kind + place
    steps = len(PLAN[0])
    words = []
    for n in range(steps):
        word = PLAN[0][n]
        for c in range(1, len(PLAN)):
            word = jnp.where(kind == c, PLAN[c][n], word)
        words.append(word)

    def word_of(turn, place_in_turn):
        word = words[place_in_turn]
        for i in range(1, steps // TURN):
            word = jnp.where(turn == i, words[i * TURN + place_in_turn], word)
        return word

    def relay(code):
        slot = lax.rem(code // 32, 64)
        part = lax.rem(code // 16, 2)
        directions = lax.rem(code, 16)
        back = slot // HEADS

        @pl.when((code >= 2048) & (back <= seq))
        def _():
            @pl.when(slot >= HEADS)
            def _():
                arrived(slot, part).wait_recv()

            for direction in range(4):

                @pl.when(lax.rem(directions // (1 << direction), 2) == 1)
                def _():
                    hand_on(slot, part, direction).start()

    def sent(code):
        slot = lax.rem(code // 32, 64)
        part = lax.rem(code // 16, 2)
        directions = lax.rem(code, 16)

        @pl.when((code >= 2048) & (slot // HEADS <= seq))
        def _():
            for direction in range(4):

                @pl.when(lax.rem(directions // (1 << direction), 2) == 1)
                def _():
                    hand_on(slot, part, direction).wait_send()

    for copy in locals_:
        copy.wait()
    for copy in swaps:
        copy.wait()

    for n in range(FIRST):
        relay(words[n] // 64)
    for head in range(HEADS):
        attend(queries_t, window, thresholds, top, total, summed, 0, head, True)

    def step(turn, _):
        for place_in_turn in range(TURN):
            word = word_of(turn, place_in_turn)

            @pl.when(turn * TURN + place_in_turn >= FIRST)
            def _():
                relay(word // 64)

            slot = lax.rem(word, 64)

            @pl.when((slot >= HEADS) & (slot // HEADS <= seq))
            def _():
                back, head = slot // HEADS, lax.rem(slot, HEADS)
                attend(queries_t, window, thresholds, top, total, summed, back, head, False)

        return 0

    lax.fori_loop(0, steps // TURN, step, 0)

    for head in range(HEADS):
        for member in range(GROUP):
            span = slice(member * TOK, (member + 1) * TOK)
            inverse = 1.0 / total[head, :, span]
            result[:, head * GROUP + member, :] = (summed[head, :, span] * inverse).T
    o_ref[...] = result[...].astype(jnp.bfloat16)

    def finish(turn, _):
        for place_in_turn in range(TURN):
            sent(word_of(turn, place_in_turn) // 64)
        return 0

    lax.fori_loop(0, steps // TURN, finish, 0)


def body(queries, keys, values, doc_start, tile_list, tile_count):
    keys_t = jnp.swapaxes(keys, 0, 1)
    values_t = jnp.swapaxes(values, 0, 1)
    vmem = pl.BlockSpec(memory_space=pltpu.VMEM)
    hbm = pl.BlockSpec(memory_space=pltpu.HBM)
    lanes = GROUP * TOK
    return pl.pallas_call(
        kernel,
        out_shape=jax.ShapeDtypeStruct(queries.shape, jnp.bfloat16),
        in_specs=[vmem, hbm, hbm, vmem, vmem, pl.BlockSpec(memory_space=pltpu.SMEM)],
        out_specs=vmem,
        scratch_shapes=[
            pltpu.VMEM((BACK, HEADS, 2, TOK, HD), jnp.bfloat16),
            pltpu.VMEM((HEADS, HD, lanes), jnp.bfloat16),
            pltpu.VMEM((24, TOK), jnp.int32),
            pltpu.VMEM((HEADS, 1, lanes), jnp.float32),
            pltpu.VMEM((HEADS, 1, lanes), jnp.float32),
            pltpu.VMEM((HEADS, HD, lanes), jnp.float32),
            pltpu.VMEM(queries.shape, jnp.float32),
            pltpu.SemaphoreType.DMA((2,)),
            pltpu.SemaphoreType.DMA((2,)),
            pltpu.SemaphoreType.DMA((2,)),
            pltpu.SemaphoreType.DMA((ENTRIES, 2, 4)),
            pltpu.SemaphoreType.DMA((ENTRIES, 2)),
        ],
        compiler_params=pltpu.CompilerParams(collective_id=0, has_side_effects=True),
    )(queries, keys_t, values_t, doc_start.reshape(1, TOK), tile_list, tile_count)


def solution(mesh):
    in_specs = (
        P("seq", "head", None),
        P(("seq", "head"), None, None),
        P(("seq", "head"), None, None),
        P("seq"),
        P("seq", None),
        P("seq"),
    )
    return jax.shard_map(
        body, mesh=mesh, in_specs=in_specs, out_specs=P("seq", "head", None), check_vma=False
    )
```

```python
import jax
import jax.numpy as jnp
from jax import lax
from jax.experimental import pallas as pl
from jax.experimental.pallas import tpu as pltpu
from jax.sharding import PartitionSpec as P

TILE = 128
REACH = 8
BACK = REACH + 1
SIDE = 4
HEADS = 4
GROUP = 4
TOK = 256
HD = 128
ENTRIES = BACK * HEADS
FIRST = 2
TURN = 5
LAG = 3
NEG = -1e30
FAR = 1 << 20
MESH = pl.DeviceIdType.MESH

PLAN = (
    (133376, 134400, 137664, 138688, 131264, 132288, 166336, 167377, 135360, 136384, 170368, 162048, 143680, 171411, 163087, 144704, 198662, 157952, 145472, 199713, 158989, 202752, 146503, 160128, 194624, 139264, 151680, 176256, 140292, 161152, 203790, 141411, 152704, 195658, 142431, 177280, 180741, 178176, 190528, 181782, 179224, 147456, 191552, 149527, 153885, 192576, 188928, 172032, 193600, 148480, 189982, 164168, 150556, 186368, 154889, 155648, 168203, 173076, 184320, 156672, 196608, 165196, 182288, 187392, 174107, 169234, 175104, 200725, 183321, 197632, 185376, 26, 201762, 0, 0, 0, 0, 0, 0, 0),
    (137536, 138560, 133440, 134464, 135424, 136448, 170112, 131392, 132416, 171155, 145408, 166080, 146439, 155904, 167121, 139328, 156940, 168128, 140356, 159872, 169170, 174592, 160910, 164096, 175637, 161792, 165136, 143616, 162831, 141376, 188608, 144646, 142400, 189632, 158080, 151557, 28, 196736, 147712, 152586, 197760, 159136, 153869, 176320, 192640, 154891, 190592, 148744, 202752, 177344, 184342, 149824, 191616, 193693, 203806, 180224, 185344, 150883, 26, 186432, 194560, 198665, 181248, 178200, 199713, 187456, 195584, 200731, 31, 182272, 179200, 201751, 34, 183296, 172057, 173076, 0, 0, 0, 0),
    (131392, 132416, 135488, 136512, 137472, 138496, 145472, 164032, 146503, 133440, 134464, 165072, 141312, 168320, 142341, 160000, 169362, 139584, 161038, 170432, 140612, 161792, 171475, 174144, 162831, 166336, 175189, 155776, 167377, 147456, 200832, 176128, 156812, 192640, 148488, 182272, 201890, 177152, 183318, 193689, 149504, 151582, 202880, 196608, 152586, 172032, 150537, 187008, 203939, 197632, 188448, 173076, 184320, 188059, 198656, 180224, 153600, 185370, 199680, 178209, 157952, 154635, 189468, 158976, 181261, 24, 194560, 143360, 190464, 179223, 195615, 144390, 191517, 0, 0, 0, 0, 0, 0, 0),
    (135424, 136448, 137472, 138496, 139264, 168128, 140292, 131328, 132352, 133376, 134400, 169170, 143360, 161792, 170432, 144390, 162831, 171456, 153875, 155904, 172032, 164288, 156940, 154891, 165312, 191120, 141312, 166208, 192157, 142341, 167232, 160145, 173056, 157696, 202836, 161166, 147712, 203840, 158720, 194723, 178765, 196800, 195743, 148736, 188616, 184832, 145408, 179799, 186496, 176128, 182784, 197856, 200704, 146439, 174080, 189632, 185884, 151680, 183834, 198720, 177177, 175104, 187542, 201749, 149504, 199771, 34, 152704, 192545, 150538, 193545, 180254, 181272, 0, 0, 0, 0, 0, 0, 0),
    (133376, 134400, 137664, 138688, 131264, 132288, 166336, 167377, 135360, 136384, 170368, 162048, 143680, 171411, 163087, 144704, 198662, 157952, 199713, 145472, 158989, 202752, 146503, 160128, 194624, 139264, 151680, 176256, 140292, 161152, 203790, 141411, 152704, 195658, 142400, 180767, 177285, 178176, 149504, 190550, 179223, 181760, 191576, 153856, 147456, 150528, 192605, 164169, 188928, 193630, 154891, 189952, 148508, 172032, 184328, 186368, 165200, 155648, 168192, 173076, 156672, 169216, 196620, 174098, 182272, 187419, 175104, 185365, 200730, 183321, 197664, 201762, 0, 0, 0, 0, 0, 0, 0, 0),
    (137536, 138560, 133440, 134464, 170112, 135424, 136448, 171155, 131392, 132416, 145408, 166080, 155904, 146432, 167111, 156945, 139328, 168140, 159872, 140352, 169156, 18, 160896, 174592, 164110, 161792, 175616, 165141, 16, 162816, 143616, 188623, 158080, 141376, 144640, 189638, 28, 159104, 142400, 151552, 196749, 147717, 152576, 197770, 192640, 153856, 176352, 148744, 154880, 177355, 184342, 202752, 190592, 193694, 149824, 180224, 185370, 203776, 191651, 194589, 150848, 186441, 178176, 198656, 187483, 195615, 199680, 181281, 179224, 200704, 182295, 172032, 183321, 201762, 173076, 0, 0, 0, 0, 0),
    (131392, 132416, 135488, 136512, 137472, 138496, 164032, 145472, 165056, 146512, 133440, 134471, 168320, 141312, 160000, 169362, 142341, 161024, 170446, 139584, 171456, 161811, 140612, 166336, 162816, 174159, 167377, 175168, 155797, 200832, 147456, 156812, 192640, 176128, 182272, 201890, 148480, 183304, 172057, 177152, 151574, 193664, 196638, 152586, 202880, 149504, 178176, 173076, 197632, 187040, 203939, 150528, 180233, 198656, 184320, 188059, 199713, 185344, 153600, 188442, 157952, 181272, 154635, 179223, 158989, 189468, 194560, 143360, 190464, 195615, 144390, 191517, 0, 0, 0, 0, 0, 0, 0, 0),
    (135424, 136448, 137472, 138496, 139264, 168128, 140288, 169156, 131328, 132352, 133376, 134418, 143360, 170432, 161792, 144390, 171456, 162835, 172047, 164288, 155904, 153856, 165328, 156940, 173056, 166208, 191124, 154891, 167232, 192145, 141341, 202816, 160128, 142341, 157696, 203840, 161187, 178752, 186496, 158720, 194702, 13, 147712, 188608, 195743, 179799, 196800, 184832, 145408, 148744, 189632, 176156, 174080, 187547, 200704, 146439, 182784, 197824, 185888, 151680, 175130, 198720, 177173, 183808, 199766, 201728, 149529, 192545, 152738, 193546, 150558, 180233, 181272, 0, 0, 0, 0, 0, 0, 0),
    (133376, 134400, 137664, 138688, 131264, 132288, 166336, 167377, 135360, 136384, 170368, 162048, 143680, 171411, 163087, 144704, 198662, 157952, 199713, 145472, 158989, 202752, 146503, 160128, 194624, 139264, 151680, 176256, 140292, 161152, 203790, 141411, 152704, 195658, 142400, 180767, 177285, 178176, 149504, 190550, 179223, 181760, 191576, 147456, 153856, 150528, 192605, 9, 172032, 188928, 193630, 164160, 189952, 148508, 8, 186368, 154880, 184331, 196608, 173056, 155668, 168192, 187419, 165184, 156672, 182288, 174092, 169216, 197650, 175104, 185376, 200725, 183322, 201753, 34, 0, 0, 0, 0, 0),
    (137536, 138560, 133440, 134464, 170112, 135424, 136448, 171155, 131392, 132416, 145408, 166080, 155904, 146432, 167111, 156945, 139328, 168140, 159872, 140352, 169156, 18, 160896, 174592, 164110, 161792, 175616, 165141, 16, 162816, 143616, 188623, 158080, 141376, 144640, 189638, 28, 159104, 142400, 151552, 196749, 147717, 152576, 197770, 192640, 153856, 176352, 148744, 154880, 190603, 184320, 202752, 177366, 193694, 149824, 191645, 185370, 203776, 180259, 194560, 150848, 186441, 195615, 198656, 181272, 178176, 199680, 187489, 27, 179200, 200704, 182295, 201728, 183330, 25, 172032, 173076, 0, 0, 0),
    (131392, 132416, 135488, 136512, 137472, 138496, 164032, 145472, 165056, 146512, 133440, 134471, 168320, 141312, 160000, 169362, 142341, 161024, 170446, 139584, 171456, 161811, 140612, 166336, 162816, 174159, 167377, 175168, 155797, 200832, 147456, 156812, 192640, 176128, 182272, 201890, 148480, 183304, 193689, 177152, 151582, 202880, 196630, 152586, 172032, 149504, 188416, 203939, 197632, 187040, 173076, 150528, 180233, 198656, 184320, 188059, 199713, 185344, 153600, 178202, 157952, 189468, 154635, 181272, 158989, 143360, 190464, 194560, 179223, 195615, 144390, 191517, 0, 0, 0, 0, 0, 0, 0, 0),
    (135424, 136448, 137472, 138496, 139264, 168128, 140288, 169156, 131328, 132352, 133376, 134418, 143360, 170432, 161792, 144390, 171456, 162835, 172047, 164288, 155904, 153856, 165328, 156940, 173056, 166208, 191124, 154891, 167232, 192145, 141341, 202816, 160128, 142341, 157696, 203840, 161187, 178766, 196800, 158720, 194701, 147712, 188608, 195743, 179799, 186496, 184832, 145408, 148744, 197824, 176160, 174080, 189660, 200704, 146432, 182791, 198720, 185882, 151680, 175104, 187541, 177179, 183808, 199744, 201750, 149529, 192545, 152738, 193546, 150528, 180254, 9, 181272, 0, 0, 0, 0, 0, 0, 0),
    (133376, 134400, 137664, 138688, 131264, 132288, 166336, 167377, 135360, 136384, 170368, 162048, 143680, 171411, 163087, 144704, 198662, 157952, 199713, 145472, 158989, 202752, 146503, 160128, 194624, 139264, 151680, 176256, 140292, 161152, 203790, 141411, 152704, 195658, 142400, 180767, 177285, 178176, 149504, 190550, 179223, 181760, 191576, 153856, 150557, 192585, 172032, 188928, 193630, 164160, 147456, 189980, 186368, 154891, 148480, 184328, 173076, 168192, 196608, 165200, 155648, 182272, 174080, 187419, 156672, 169228, 175104, 185344, 200722, 21, 183296, 197658, 25, 201760, 34, 0, 0, 0, 0, 0),
    (137536, 138560, 133440, 134464, 170112, 135424, 136448, 171155, 131392, 132416, 145408, 166080, 155904, 146432, 167111, 156945, 139328, 168140, 159872, 140352, 169156, 18, 160896, 174592, 164110, 161792, 175616, 165141, 16, 162816, 143616, 188623, 158080, 144640, 189638, 28, 159104, 141376, 151552, 196749, 147712, 142400, 152576, 197765, 10, 192640, 153856, 176352, 148744, 154880, 190603, 184320, 202752, 177366, 193694, 149824, 191645, 185370, 203776, 180259, 194560, 150848, 186441, 195615, 198656, 181272, 178176, 199680, 187489, 27, 179200, 200704, 182295, 201728, 183330, 25, 172032, 173076, 0, 0),
    (131392, 132416, 135488, 136512, 137472, 138496, 164032, 145472, 165056, 146512, 133440, 134471, 168320, 141312, 160000, 169362, 142341, 161024, 170446, 139584, 171456, 161811, 140612, 166336, 162816, 174159, 167377, 175168, 155797, 200832, 147456, 156812, 192640, 176128, 182272, 201890, 148480, 183304, 193689, 177152, 151582, 202880, 196630, 152586, 172032, 197632, 188448, 203939, 149504, 187008, 173076, 150528, 180233, 198656, 184320, 188059, 199713, 185344, 178202, 153600, 157952, 189468, 181272, 158989, 154624, 179211, 190464, 194583, 143360, 195615, 144390, 191517, 0, 0, 0, 0, 0, 0, 0, 0),
    (135424, 136448, 137472, 138496, 139264, 168128, 140288, 169156, 131328, 132352, 133376, 134418, 143360, 170432, 161792, 144390, 171456, 162835, 172047, 164288, 155904, 153856, 165328, 156940, 173056, 166208, 191124, 154891, 167232, 192145, 141341, 202816, 160128, 142341, 203840, 161187, 178752, 157710, 196800, 194688, 147712, 158733, 188608, 195743, 179776, 186496, 184855, 148744, 197824, 176160, 174080, 189660, 200704, 145408, 182784, 198720, 185882, 175125, 187520, 177152, 151707, 183830, 199744, 201728, 146457, 192512, 149537, 34, 193536, 152711, 30, 180224, 150538, 9, 181272, 0, 0, 0, 0, 0),
    (131328, 132352, 137344, 138368, 135488, 136512, 166336, 167377, 170368, 133568, 134592, 162048, 143680, 171411, 163087, 144704, 198662, 157952, 199680, 145505, 158989, 202752, 146503, 160128, 194624, 139264, 151680, 176256, 140292, 161152, 203790, 141411, 152704, 195658, 142400, 180767, 177285, 178176, 149504, 190550, 179223, 181760, 191576, 172032, 150557, 192585, 164160, 188928, 193630, 153856, 147456, 184320, 154891, 186368, 189952, 148508, 173056, 196616, 168212, 165184, 187392, 155648, 182288, 174107, 169234, 197632, 175136, 185344, 200725, 156672, 183322, 201740, 25, 34, 0, 0, 0, 0, 0, 0),
    (131392, 132416, 137472, 138496, 135424, 136448, 170112, 171155, 133440, 134464, 166080, 143424, 155904, 167121, 144454, 156928, 168128, 174604, 159872, 169170, 175637, 160896, 164096, 141582, 161792, 165136, 142597, 162816, 188608, 151567, 158080, 189660, 152586, 159104, 196736, 153869, 192640, 197760, 154912, 11, 147712, 176320, 202752, 184320, 190592, 149824, 178176, 177344, 203798, 35, 193664, 191616, 150878, 29, 148736, 180224, 198656, 145417, 185344, 186432, 199688, 146458, 139264, 181248, 200737, 7, 179200, 187456, 172056, 194560, 182272, 201751, 27, 195584, 183330, 173087, 140313, 20, 4, 0),
    (135424, 136448, 131392, 132416, 137536, 138560, 133440, 134464, 164032, 139328, 165056, 140368, 4, 168320, 160000, 169362, 161038, 170432, 141312, 161792, 171475, 142341, 182272, 166336, 174144, 162831, 167377, 151872, 183296, 200857, 175189, 155776, 192640, 152906, 187008, 201890, 176128, 156812, 193664, 147678, 177152, 188032, 202902, 196635, 172032, 143360, 188416, 197664, 203939, 180224, 184320, 144384, 173062, 178196, 157952, 198656, 148672, 189448, 28, 185344, 199680, 145690, 159009, 181261, 149528, 146695, 194560, 150528, 179209, 23, 153600, 190464, 195584, 154655, 11, 191517, 0, 0, 0, 0),
    (133376, 134400, 135424, 136448, 168128, 131328, 132352, 162048, 169170, 163087, 137472, 138496, 170432, 139264, 191104, 171456, 140307, 4, 192128, 145664, 164317, 194688, 146695, 165328, 157696, 141312, 166208, 158733, 142336, 167237, 195712, 172032, 202833, 31, 147456, 203875, 184832, 173076, 196800, 143360, 176128, 148488, 188608, 200704, 178752, 186496, 144384, 185862, 179776, 197850, 153728, 177152, 174103, 189664, 154752, 201728, 182784, 198742, 151580, 175104, 187531, 160034, 199744, 152597, 183808, 192539, 33, 161024, 193546, 25, 155648, 180224, 149518, 156702, 181248, 150540, 24, 9, 0, 0),
    (131200, 132224, 135360, 136384, 163904, 137408, 138432, 164944, 133248, 134272, 168000, 155776, 141376, 169042, 156812, 142400, 198661, 161920, 199680, 143457, 162959, 202752, 144454, 159872, 165888, 139264, 147584, 166929, 140292, 160896, 194638, 170048, 148616, 176256, 171091, 157824, 203811, 151552, 158861, 195648, 145439, 180736, 177302, 146439, 181760, 190552, 152576, 149514, 191552, 178205, 188928, 192576, 179223, 150537, 193600, 153694, 184320, 196608, 172032, 189980, 186368, 154699, 185370, 187392, 173083, 182272, 200724, 174080, 183321, 197632, 175136, 21, 201762, 0, 0, 0, 0, 0, 0, 0),
    (137280, 138304, 135232, 136256, 131136, 132160, 163968, 143360, 133184, 134208, 165008, 144390, 170112, 172096, 159744, 171155, 145472, 160782, 168128, 146503, 155776, 169170, 173120, 156820, 166028, 176128, 139264, 167057, 149504, 188608, 177152, 140310, 189636, 150528, 157852, 196745, 151552, 158861, 174144, 152576, 192650, 197792, 202752, 184320, 175189, 178752, 193694, 190592, 179776, 147479, 191645, 203776, 185379, 186458, 148488, 198656, 187483, 194560, 180224, 199713, 141312, 182272, 200704, 195615, 183296, 201753, 142370, 181248, 161797, 153624, 162831, 154635, 0, 0, 0, 0, 0, 0, 0, 0),
    (133184, 134208, 131136, 132160, 135232, 136256, 137280, 138304, 168128, 145472, 169152, 146514, 7, 163968, 143424, 157696, 164992, 144464, 6, 147584, 169984, 139328, 158733, 171008, 140371, 148612, 166080, 141384, 159744, 167104, 142417, 5, 151552, 200832, 180800, 160782, 192640, 153600, 152586, 201856, 176674, 155776, 193664, 154654, 11, 156800, 202880, 177676, 22, 149632, 203904, 181859, 150680, 198656, 196617, 161920, 199680, 197665, 32, 172032, 184320, 182848, 162959, 185344, 183898, 173081, 186900, 190464, 188416, 187931, 189468, 194560, 178176, 174080, 195615, 191517, 175125, 179223, 0, 0),
    (135168, 136192, 133120, 134144, 166080, 141312, 155776, 131072, 132096, 167104, 142353, 156800, 137216, 138245, 139264, 168128, 159884, 140292, 169152, 160914, 143360, 164046, 161792, 144390, 165056, 162832, 145408, 194639, 157824, 146439, 195648, 158879, 176704, 170189, 180352, 153600, 171219, 181400, 177728, 202816, 186902, 154635, 203840, 187939, 151552, 178267, 184832, 152586, 196800, 172032, 147456, 179287, 185882, 148480, 197824, 173064, 32, 174080, 198720, 200724, 149504, 199777, 182912, 175125, 183961, 150537, 201762, 192512, 188416, 189468, 190464, 193566, 191517, 0, 0, 0, 0, 0, 0, 0),
)


def attend(queries_t, window, thresholds, top, total, summed, back, head, own):
    scale = HD ** (-0.5) * 1.4426950408889634
    key_tile = window[back, head, 0]
    value_tile = window[back, head, 1]
    iota = lax.broadcasted_iota(jnp.int32, (TILE, TOK), 0)
    seen = []
    for half in range(2):
        mask = iota >= thresholds[pl.ds(back * 2 + half, 1), :]
        if own:
            mask = mask & (iota + half * TILE <= lax.broadcasted_iota(jnp.int32, (TILE, TOK), 1))
        seen.append(mask)
    spans = [slice(member * TOK, (member + 1) * TOK) for member in range(GROUP)]
    if not own:
        old_tops = [top[head, :, span] for span in spans]
        old_totals = [total[head, :, span] for span in spans]
    raw = [
        jnp.dot(key_tile, queries_t[head, :, span], preferred_element_type=jnp.float32)
        for span in spans
    ]
    tops, totals, factors, products = [], [], [], []
    for member in range(GROUP):
        scores = jnp.concatenate(
            [
                jnp.where(seen[half], raw[member][half * TILE : (half + 1) * TILE], NEG)
                for half in range(2)
            ],
            axis=0,
        )
        new_top = jnp.max(scores, axis=0, keepdims=True)
        if not own:
            new_top = jnp.maximum(old_tops[member], new_top)
        scaled_top = new_top * scale
        weights = jnp.exp2(scores * scale - scaled_top)
        weight_sum = jnp.sum(weights, axis=0, keepdims=True)
        products.append(
            lax.dot_general(
                value_tile,
                weights.astype(jnp.bfloat16),
                (((0,), (0,)), ((), ())),
                preferred_element_type=jnp.float32,
            )
        )
        if not own:
            factors.append(jnp.exp2(old_tops[member] * scale - scaled_top))
            weight_sum = old_totals[member] * factors[member] + weight_sum
        tops.append(new_top)
        totals.append(weight_sum)
    for member, span in enumerate(spans):
        top[head, :, span] = tops[member]
        total[head, :, span] = totals[member]
        if own:
            summed[head, :, span] = products[member]
        else:
            summed[head, :, span] = summed[head, :, span] * factors[member] + products[member]


def kernel(
    q_ref,
    k_ref,
    v_ref,
    start_ref,
    list_ref,
    count_ref,
    o_ref,
    window,
    queries_t,
    thresholds,
    top,
    total,
    summed,
    result,
    q_here,
    kv_here,
    swapped,
    o_here,
    in_sem,
    out_sem,
    swap_send,
    swap_recv,
    send_sem,
    recv_sem,
):
    seq = lax.axis_index("seq")
    core = lax.axis_index("head")
    devices = lax.axis_size("seq")
    place = lax.rem(seq, SIDE)
    row_first = seq - place
    neighbours = (
        row_first + lax.rem(place + 1, SIDE),
        row_first + lax.rem(place + SIDE - 1, SIDE),
        lax.rem(seq + SIDE, devices),
        lax.rem(seq + devices - SIDE, devices),
    )
    last = place == SIDE - 1
    none = place == 0
    shifts = (
        jnp.where(last, 1 - SIDE, 1),
        jnp.where(none, SIDE - 1, -1),
        SIDE,
        -SIDE,
    )

    row = seq // SIDE
    rows = devices // SIDE
    not_last = row < rows - 1
    not_first = row > 0

    barrier = pltpu.get_barrier_semaphore()
    for where, there in zip(neighbours, (None, None, not_last, not_first)):

        def greet(where=where):
            pl.semaphore_signal(barrier, inc=1, device_id=(where, core), device_id_type=MESH)

        if there is None:
            greet()
        else:
            pl.when(there)(greet)

    ins = []
    for part, (ref, here) in enumerate(
        ((k_ref, kv_here.at[0]), (v_ref, kv_here.at[1]), (q_ref, q_here))
    ):
        ins.append(pltpu.make_async_copy(ref, here, in_sem.at[part]))
    for copy in ins:
        copy.start()

    kind = jnp.where(
        row == rows - 1,
        5 * SIDE,
        jnp.where(row == rows - 2, 4 * SIDE, lax.rem(row, SIDE) * SIDE),
    )
    kind = kind + place
    steps = len(PLAN[0])
    words = []
    for n in range(steps):
        word = PLAN[0][n]
        for c in range(1, len(PLAN)):
            word = jnp.where(kind == c, PLAN[c][n], word)
        words.append(word)

    def word_of(turn, place_in_turn):
        word = words[place_in_turn]
        for i in range(1, steps // TURN):
            word = jnp.where(turn == i, words[i * TURN + place_in_turn], word)
        return word

    tile_row = lax.broadcasted_iota(jnp.int32, (24, 1), 0)
    back_of = tile_row // 2
    half_of = tile_row - 2 * back_of
    tile_id = 2 * (seq - back_of) + half_of
    slots = list_ref.shape[1]
    listed = (list_ref[...] == tile_id) & (
        lax.broadcasted_iota(jnp.int32, (1, slots), 1) < count_ref[0]
    )
    live = jnp.max(jnp.where(listed, 1.0, 0.0), axis=1, keepdims=True)
    low = start_ref[...] - seq * TOK + (back_of * TOK - half_of * TILE)
    thresholds[...] = jnp.where(live > 0.5, low, FAR)
    for part in range(2):
        ins[part].wait()
        for mine in range(2):

            @pl.when(core == mine)
            def _():
                for head in range(HEADS):
                    window[0, head, part, mine * TILE : (mine + 1) * TILE, :] = kv_here[
                        part, :, mine * HEADS + head, :
                    ]
                    swapped[part, head] = kv_here[part, :, (1 - mine) * HEADS + head, :]

    pl.semaphore_signal(barrier, inc=1, device_id=(seq, 1 - core), device_id_type=MESH)
    pl.semaphore_wait(
        barrier, 3 + jnp.where(not_last, 1, 0) + jnp.where(not_first, 1, 0)
    )
    swaps = []
    for part in range(2):
        swaps.append(
            pltpu.make_async_remote_copy(
                src_ref=swapped.at[part],
                dst_ref=window.at[0, :, part, pl.ds(core * TILE, TILE), :],
                send_sem=swap_send.at[part],
                recv_sem=swap_recv.at[part],
                device_id=(seq, 1 - core),
                device_id_type=MESH,
            )
        )
    for copy in swaps:
        copy.start()

    ins[2].wait()
    for head in range(HEADS):
        for member in range(GROUP):
            queries_t[head, :, member * TOK : (member + 1) * TOK] = q_here[
                :, head * GROUP + member, :
            ].T

    def hand_on(n, back, head, part, direction):
        there = back + shifts[direction]
        return pltpu.make_async_remote_copy(
            src_ref=window.at[back, head, part],
            dst_ref=window.at[there, head, part],
            send_sem=send_sem.at[n, direction],
            recv_sem=recv_sem.at[there * HEADS + head, part],
            device_id=(neighbours[direction], core),
            device_id_type=MESH,
        )

    def wait_for(n, back, head, part, direction):
        return pltpu.make_async_remote_copy(
            src_ref=window.at[back, head, part],
            dst_ref=window.at[back, head, part],
            send_sem=send_sem.at[n, direction],
            recv_sem=recv_sem.at[back * HEADS + head, part],
            device_id=(neighbours[0], core),
            device_id_type=MESH,
        )

    def relay(n, code):
        slot = lax.rem(code // 32, 64)
        part = lax.rem(code // 16, 2)
        directions = lax.rem(code, 16)
        back, head = slot // HEADS, lax.rem(slot, HEADS)

        @pl.when((code >= 2048) & (back <= seq))
        def _():
            @pl.when(slot >= HEADS)
            def _():
                wait_for(n, back, head, part, 0).wait_recv()

            for direction in range(4):

                @pl.when(lax.rem(directions // (1 << direction), 2) == 1)
                def _():
                    hand_on(n, back, head, part, direction).start()

    def sent(n, code):
        slot = lax.rem(code // 32, 64)
        part = lax.rem(code // 16, 2)
        directions = lax.rem(code, 16)
        back, head = slot // HEADS, lax.rem(slot, HEADS)

        @pl.when((directions > 0) & (back <= seq))
        def _():
            for direction in range(4):

                @pl.when(lax.rem(directions // (1 << direction), 2) == 1)
                def _():
                    wait_for(n, back, head, part, direction).wait_send()

    for copy in swaps:
        copy.wait()

    for n in range(FIRST):
        relay(n, words[n] // 64)
    for head in range(HEADS):
        attend(queries_t, window, thresholds, top, total, summed, 0, head, True)

    def step(turn, _):
        for place_in_turn in range(TURN):
            n = turn * TURN + place_in_turn
            word = word_of(turn, place_in_turn)

            @pl.when(n >= FIRST)
            def _():
                relay(n, word // 64)

            slot = lax.rem(word, 64)

            @pl.when((slot >= HEADS) & (slot // HEADS <= seq))
            def _():
                back, head = slot // HEADS, lax.rem(slot, HEADS)
                attend(queries_t, window, thresholds, top, total, summed, back, head, False)

            @pl.when(turn >= LAG)
            def _():
                sent(n - LAG * TURN, word_of(turn - LAG, place_in_turn) // 64)

        return 0

    lax.fori_loop(0, steps // TURN, step, 0)

    outs = []
    for half in range(2):
        rows_out = slice(half * 128, (half + 1) * 128)
        for head in range(HEADS):
            for member in range(GROUP):
                span = slice(member * TOK + half * 128, member * TOK + (half + 1) * 128)
                inverse = 1.0 / total[head, :, span]
                result[rows_out, head * GROUP + member, :] = (summed[head, :, span] * inverse).T
        o_here[rows_out] = result[rows_out].astype(jnp.bfloat16)
        outs.append(
            pltpu.make_async_copy(o_here.at[rows_out], o_ref.at[rows_out], out_sem.at[half])
        )
        if half > 0:
            outs[half - 1].start()
    outs[-1].start()

    def finish(turn, _):
        for place_in_turn in range(TURN):
            sent(turn * TURN + place_in_turn, word_of(turn, place_in_turn) // 64)
        return 0

    lax.fori_loop(steps // TURN - LAG, steps // TURN, finish, 0)
    for copy in outs:
        copy.wait()


def body(queries, keys, values, doc_start, tile_list, tile_count):
    vmem = pl.BlockSpec(memory_space=pltpu.VMEM)
    hbm = pl.BlockSpec(memory_space=pltpu.HBM)
    lanes = GROUP * TOK
    return pl.pallas_call(
        kernel,
        out_shape=jax.ShapeDtypeStruct(queries.shape, jnp.bfloat16),
        in_specs=[hbm, hbm, hbm, vmem, vmem, pl.BlockSpec(memory_space=pltpu.SMEM)],
        out_specs=hbm,
        scratch_shapes=[
            pltpu.VMEM((BACK, HEADS, 2, TOK, HD), jnp.bfloat16),
            pltpu.VMEM((HEADS, HD, lanes), jnp.bfloat16),
            pltpu.VMEM((24, TOK), jnp.int32),
            pltpu.VMEM((HEADS, 1, lanes), jnp.float32),
            pltpu.VMEM((HEADS, 1, lanes), jnp.float32),
            pltpu.VMEM((HEADS, HD, lanes), jnp.float32),
            pltpu.VMEM(queries.shape, jnp.float32),
            pltpu.VMEM(queries.shape, jnp.bfloat16),
            pltpu.VMEM((2, TILE, 2 * HEADS, HD), jnp.bfloat16),
            pltpu.VMEM((2, HEADS, TILE, HD), jnp.bfloat16),
            pltpu.VMEM(queries.shape, jnp.bfloat16),
            pltpu.SemaphoreType.DMA((3,)),
            pltpu.SemaphoreType.DMA((2,)),
            pltpu.SemaphoreType.DMA((2,)),
            pltpu.SemaphoreType.DMA((2,)),
            pltpu.SemaphoreType.DMA((len(PLAN[0]), 4)),
            pltpu.SemaphoreType.DMA((ENTRIES, 2)),
        ],
        compiler_params=pltpu.CompilerParams(collective_id=0, has_side_effects=True),
    )(queries, keys, values, doc_start.reshape(1, TOK), tile_list, tile_count)


def solution(mesh):
    in_specs = (
        P("seq", "head", None),
        P(("seq", "head"), None, None),
        P(("seq", "head"), None, None),
        P("seq"),
        P("seq", None),
        P("seq"),
    )
    return jax.shard_map(
        body, mesh=mesh, in_specs=in_specs, out_specs=P("seq", "head", None), check_vma=False
    )
```

```python
import jax
import jax.numpy as jnp
from jax import lax
from jax.experimental import pallas as pl
from jax.experimental.pallas import tpu as pltpu
from jax.sharding import PartitionSpec as P

TILE = 128
REACH = 8
BACK = REACH + 1
SIDE = 4
HEADS = 4
GROUP = 4
TOK = 256
HD = 128
ENTRIES = BACK * HEADS
FIRST = 2
TURN = 10
LAG = 2
NEG = -1e30
FAR = 1 << 20
MESH = pl.DeviceIdType.MESH

PLAN = (
    (133376, 134400, 137664, 138688, 131264, 132288, 166336, 167377, 135360, 136384, 170368, 162048, 143680, 171411, 163087, 144704, 198662, 157952, 145472, 199713, 158989, 202752, 146503, 160128, 194624, 139264, 151680, 176256, 140292, 161152, 203790, 141411, 152704, 195658, 142431, 177280, 180741, 178176, 190528, 181782, 179224, 147456, 191552, 149527, 153885, 192576, 188928, 172032, 193600, 148480, 189982, 164168, 150556, 186368, 154889, 155648, 168203, 173076, 184320, 156672, 196608, 165196, 182288, 187392, 174107, 169234, 175104, 200725, 183321, 197632, 185376, 26, 201762, 0, 0, 0, 0, 0, 0, 0),
    (137536, 138560, 133440, 134464, 135424, 136448, 170112, 131392, 132416, 171155, 145408, 166080, 146439, 155904, 167121, 139328, 156940, 168128, 140356, 159872, 169170, 174592, 160910, 164096, 175637, 161792, 165136, 143616, 162831, 141376, 188608, 144646, 142400, 189632, 158080, 151557, 28, 196736, 147712, 152586, 197760, 159136, 153869, 176320, 192640, 154891, 190592, 148744, 202752, 177344, 184342, 149824, 191616, 193693, 203806, 180224, 185344, 150883, 26, 186432, 194560, 198665, 181248, 178200, 199713, 187456, 195584, 200731, 31, 182272, 179200, 201751, 34, 183296, 172057, 173076, 0, 0, 0, 0),
    (131392, 132416, 135488, 136512, 137472, 138496, 145472, 164032, 146503, 133440, 134464, 165072, 141312, 168320, 142341, 160000, 169362, 139584, 161038, 170432, 140612, 161792, 171475, 174144, 162831, 166336, 175189, 155776, 167377, 147456, 200832, 176128, 156812, 192640, 148488, 182272, 201890, 177152, 183318, 193689, 149504, 151582, 202880, 196608, 152586, 172032, 150537, 187008, 203939, 197632, 188448, 173076, 184320, 188059, 198656, 180224, 153600, 185370, 199680, 178209, 157952, 154635, 189468, 158976, 181261, 24, 194560, 143360, 190464, 179223, 195615, 144390, 191517, 0, 0, 0, 0, 0, 0, 0),
    (135424, 136448, 137472, 138496, 139264, 168128, 140292, 131328, 132352, 133376, 134400, 169170, 143360, 161792, 170432, 144390, 162831, 171456, 153875, 155904, 172032, 164288, 156940, 154891, 165312, 191120, 141312, 166208, 192157, 142341, 167232, 160145, 173056, 157696, 202836, 161166, 147712, 203840, 158720, 194723, 178765, 196800, 195743, 148736, 188616, 184832, 145408, 179799, 186496, 176128, 182784, 197856, 200704, 146439, 174080, 189632, 185884, 151680, 183834, 198720, 177177, 175104, 187542, 201749, 149504, 199771, 34, 152704, 192545, 150538, 193545, 180254, 181272, 0, 0, 0, 0, 0, 0, 0),
    (133376, 134400, 137664, 138688, 131264, 132288, 166336, 167377, 135360, 136384, 170368, 162048, 143680, 171411, 163087, 144704, 198662, 157952, 199713, 145472, 158989, 202752, 146503, 160128, 194624, 139264, 151680, 176256, 140292, 161152, 203790, 141411, 152704, 195658, 142400, 180767, 177285, 178176, 149504, 190550, 179223, 181760, 191576, 153856, 147456, 150528, 192605, 164169, 188928, 193630, 154891, 189952, 148508, 172032, 184328, 186368, 165200, 155648, 168192, 173076, 156672, 169216, 196620, 174098, 182272, 187419, 175104, 185365, 200730, 183321, 197664, 201762, 0, 0, 0, 0, 0, 0, 0, 0),
    (137536, 138560, 133440, 134464, 170112, 135424, 136448, 171155, 131392, 132416, 145408, 166080, 155904, 146432, 167111, 156945, 139328, 168140, 159872, 140352, 169156, 18, 160896, 174592, 164110, 161792, 175616, 165141, 16, 162816, 143616, 188623, 158080, 141376, 144640, 189638, 28, 159104, 142400, 151552, 196749, 147717, 152576, 197770, 192640, 153856, 176352, 148744, 154880, 177355, 184342, 202752, 190592, 193694, 149824, 180224, 185370, 203776, 191651, 194589, 150848, 186441, 178176, 198656, 187483, 195615, 199680, 181281, 179224, 200704, 182295, 172032, 183321, 201762, 173076, 0, 0, 0, 0, 0),
    (131392, 132416, 135488, 136512, 137472, 138496, 164032, 145472, 165056, 146512, 133440, 134471, 168320, 141312, 160000, 169362, 142341, 161024, 170446, 139584, 171456, 161811, 140612, 166336, 162816, 174159, 167377, 175168, 155797, 200832, 147456, 156812, 192640, 176128, 182272, 201890, 148480, 183304, 172057, 177152, 151574, 193664, 196638, 152586, 202880, 149504, 178176, 173076, 197632, 187040, 203939, 150528, 180233, 198656, 184320, 188059, 199713, 185344, 153600, 188442, 157952, 181272, 154635, 179223, 158989, 189468, 194560, 143360, 190464, 195615, 144390, 191517, 0, 0, 0, 0, 0, 0, 0, 0),
    (135424, 136448, 137472, 138496, 139264, 168128, 140288, 169156, 131328, 132352, 133376, 134418, 143360, 170432, 161792, 144390, 171456, 162835, 172047, 164288, 155904, 153856, 165328, 156940, 173056, 166208, 191124, 154891, 167232, 192145, 141341, 202816, 160128, 142341, 157696, 203840, 161187, 178752, 186496, 158720, 194702, 13, 147712, 188608, 195743, 179799, 196800, 184832, 145408, 148744, 189632, 176156, 174080, 187547, 200704, 146439, 182784, 197824, 185888, 151680, 175130, 198720, 177173, 183808, 199766, 201728, 149529, 192545, 152738, 193546, 150558, 180233, 181272, 0, 0, 0, 0, 0, 0, 0),
    (133376, 134400, 137664, 138688, 131264, 132288, 166336, 167377, 135360, 136384, 170368, 162048, 143680, 171411, 163087, 144704, 198662, 157952, 199713, 145472, 158989, 202752, 146503, 160128, 194624, 139264, 151680, 176256, 140292, 161152, 203790, 141411, 152704, 195658, 142400, 180767, 177285, 178176, 149504, 190550, 179223, 181760, 191576, 147456, 153856, 150528, 192605, 9, 172032, 188928, 193630, 164160, 189952, 148508, 8, 186368, 154880, 184331, 196608, 173056, 155668, 168192, 187419, 165184, 156672, 182288, 174092, 169216, 197650, 175104, 185376, 200725, 183322, 201753, 34, 0, 0, 0, 0, 0),
    (137536, 138560, 133440, 134464, 170112, 135424, 136448, 171155, 131392, 132416, 145408, 166080, 155904, 146432, 167111, 156945, 139328, 168140, 159872, 140352, 169156, 18, 160896, 174592, 164110, 161792, 175616, 165141, 16, 162816, 143616, 188623, 158080, 141376, 144640, 189638, 28, 159104, 142400, 151552, 196749, 147717, 152576, 197770, 192640, 153856, 176352, 148744, 154880, 190603, 184320, 202752, 177366, 193694, 149824, 191645, 185370, 203776, 180259, 194560, 150848, 186441, 195615, 198656, 181272, 178176, 199680, 187489, 27, 179200, 200704, 182295, 201728, 183330, 25, 172032, 173076, 0, 0, 0),
    (131392, 132416, 135488, 136512, 137472, 138496, 164032, 145472, 165056, 146512, 133440, 134471, 168320, 141312, 160000, 169362, 142341, 161024, 170446, 139584, 171456, 161811, 140612, 166336, 162816, 174159, 167377, 175168, 155797, 200832, 147456, 156812, 192640, 176128, 182272, 201890, 148480, 183304, 193689, 177152, 151582, 202880, 196630, 152586, 172032, 149504, 188416, 203939, 197632, 187040, 173076, 150528, 180233, 198656, 184320, 188059, 199713, 185344, 153600, 178202, 157952, 189468, 154635, 181272, 158989, 143360, 190464, 194560, 179223, 195615, 144390, 191517, 0, 0, 0, 0, 0, 0, 0, 0),
    (135424, 136448, 137472, 138496, 139264, 168128, 140288, 169156, 131328, 132352, 133376, 134418, 143360, 170432, 161792, 144390, 171456, 162835, 172047, 164288, 155904, 153856, 165328, 156940, 173056, 166208, 191124, 154891, 167232, 192145, 141341, 202816, 160128, 142341, 157696, 203840, 161187, 178766, 196800, 158720, 194701, 147712, 188608, 195743, 179799, 186496, 184832, 145408, 148744, 197824, 176160, 174080, 189660, 200704, 146432, 182791, 198720, 185882, 151680, 175104, 187541, 177179, 183808, 199744, 201750, 149529, 192545, 152738, 193546, 150528, 180254, 9, 181272, 0, 0, 0, 0, 0, 0, 0),
    (133376, 134400, 137664, 138688, 131264, 132288, 166336, 167377, 135360, 136384, 170368, 162048, 143680, 171411, 163087, 144704, 198662, 157952, 199713, 145472, 158989, 202752, 146503, 160128, 194624, 139264, 151680, 176256, 140292, 161152, 203790, 141411, 152704, 195658, 142400, 180767, 177285, 178176, 149504, 190550, 179223, 181760, 191576, 153856, 150557, 192585, 172032, 188928, 193630, 164160, 147456, 189980, 186368, 154891, 148480, 184328, 173076, 168192, 196608, 165200, 155648, 182272, 174080, 187419, 156672, 169228, 175104, 185344, 200722, 21, 183296, 197658, 25, 201760, 34, 0, 0, 0, 0, 0),
    (137536, 138560, 133440, 134464, 170112, 135424, 136448, 171155, 131392, 132416, 145408, 166080, 155904, 146432, 167111, 156945, 139328, 168140, 159872, 140352, 169156, 18, 160896, 174592, 164110, 161792, 175616, 165141, 16, 162816, 143616, 188623, 158080, 144640, 189638, 28, 159104, 141376, 151552, 196749, 147712, 142400, 152576, 197765, 10, 192640, 153856, 176352, 148744, 154880, 190603, 184320, 202752, 177366, 193694, 149824, 191645, 185370, 203776, 180259, 194560, 150848, 186441, 195615, 198656, 181272, 178176, 199680, 187489, 27, 179200, 200704, 182295, 201728, 183330, 25, 172032, 173076, 0, 0),
    (131392, 132416, 135488, 136512, 137472, 138496, 164032, 145472, 165056, 146512, 133440, 134471, 168320, 141312, 160000, 169362, 142341, 161024, 170446, 139584, 171456, 161811, 140612, 166336, 162816, 174159, 167377, 175168, 155797, 200832, 147456, 156812, 192640, 176128, 182272, 201890, 148480, 183304, 193689, 177152, 151582, 202880, 196630, 152586, 172032, 197632, 188448, 203939, 149504, 187008, 173076, 150528, 180233, 198656, 184320, 188059, 199713, 185344, 178202, 153600, 157952, 189468, 181272, 158989, 154624, 179211, 190464, 194583, 143360, 195615, 144390, 191517, 0, 0, 0, 0, 0, 0, 0, 0),
    (135424, 136448, 137472, 138496, 139264, 168128, 140288, 169156, 131328, 132352, 133376, 134418, 143360, 170432, 161792, 144390, 171456, 162835, 172047, 164288, 155904, 153856, 165328, 156940, 173056, 166208, 191124, 154891, 167232, 192145, 141341, 202816, 160128, 142341, 203840, 161187, 178752, 157710, 196800, 194688, 147712, 158733, 188608, 195743, 179776, 186496, 184855, 148744, 197824, 176160, 174080, 189660, 200704, 145408, 182784, 198720, 185882, 175125, 187520, 177152, 151707, 183830, 199744, 201728, 146457, 192512, 149537, 34, 193536, 152711, 30, 180224, 150538, 9, 181272, 0, 0, 0, 0, 0),
    (131328, 132352, 137344, 138368, 135488, 136512, 166336, 167377, 170368, 133568, 134592, 162048, 143680, 171411, 163087, 144704, 198662, 157952, 199680, 145505, 158989, 202752, 146503, 160128, 194624, 139264, 151680, 176256, 140292, 161152, 203790, 141411, 152704, 195658, 142400, 180767, 177285, 178176, 149504, 190550, 179223, 181760, 191576, 172032, 150557, 192585, 164160, 188928, 193630, 153856, 147456, 184320, 154891, 186368, 189952, 148508, 173056, 196616, 168212, 165184, 187392, 155648, 182288, 174107, 169234, 197632, 175136, 185344, 200725, 156672, 183322, 201740, 25, 34, 0, 0, 0, 0, 0, 0),
    (131392, 132416, 137472, 138496, 135424, 136448, 170112, 171155, 133440, 134464, 166080, 143424, 155904, 167121, 144454, 156928, 168128, 174604, 159872, 169170, 175637, 160896, 164096, 141582, 161792, 165136, 142597, 162816, 188608, 151567, 158080, 189660, 152586, 159104, 196736, 153869, 192640, 197760, 154912, 11, 147712, 176320, 202752, 184320, 190592, 149824, 178176, 177344, 203798, 35, 193664, 191616, 150878, 29, 148736, 180224, 198656, 145417, 185344, 186432, 199688, 146458, 139264, 181248, 200737, 7, 179200, 187456, 172056, 194560, 182272, 201751, 27, 195584, 183330, 173087, 140313, 20, 4, 0),
    (135424, 136448, 131392, 132416, 137536, 138560, 133440, 134464, 164032, 139328, 165056, 140368, 4, 168320, 160000, 169362, 161038, 170432, 141312, 161792, 171475, 142341, 182272, 166336, 174144, 162831, 167377, 151872, 183296, 200857, 175189, 155776, 192640, 152906, 187008, 201890, 176128, 156812, 193664, 147678, 177152, 188032, 202902, 196635, 172032, 143360, 188416, 197664, 203939, 180224, 184320, 144384, 173062, 178196, 157952, 198656, 148672, 189448, 28, 185344, 199680, 145690, 159009, 181261, 149528, 146695, 194560, 150528, 179209, 23, 153600, 190464, 195584, 154655, 11, 191517, 0, 0, 0, 0),
    (133376, 134400, 135424, 136448, 168128, 131328, 132352, 162048, 169170, 163087, 137472, 138496, 170432, 139264, 191104, 171456, 140307, 4, 192128, 145664, 164317, 194688, 146695, 165328, 157696, 141312, 166208, 158733, 142336, 167237, 195712, 172032, 202833, 31, 147456, 203875, 184832, 173076, 196800, 143360, 176128, 148488, 188608, 200704, 178752, 186496, 144384, 185862, 179776, 197850, 153728, 177152, 174103, 189664, 154752, 201728, 182784, 198742, 151580, 175104, 187531, 160034, 199744, 152597, 183808, 192539, 33, 161024, 193546, 25, 155648, 180224, 149518, 156702, 181248, 150540, 24, 9, 0, 0),
    (131200, 132224, 135360, 136384, 163904, 137408, 138432, 164944, 133248, 134272, 168000, 155776, 141376, 169042, 156812, 142400, 198661, 161920, 199680, 143457, 162959, 202752, 144454, 159872, 165888, 139264, 147584, 166929, 140292, 160896, 194638, 170048, 148616, 176256, 171091, 157824, 203811, 151552, 158861, 195648, 145439, 180736, 177302, 146439, 181760, 190552, 152576, 149514, 191552, 178205, 188928, 192576, 179223, 150537, 193600, 153694, 184320, 196608, 172032, 189980, 186368, 154699, 185370, 187392, 173083, 182272, 200724, 174080, 183321, 197632, 175136, 21, 201762, 0, 0, 0, 0, 0, 0, 0),
    (137280, 138304, 135232, 136256, 131136, 132160, 163968, 143360, 133184, 134208, 165008, 144390, 170112, 172096, 159744, 171155, 145472, 160782, 168128, 146503, 155776, 169170, 173120, 156820, 166028, 176128, 139264, 167057, 149504, 188608, 177152, 140310, 189636, 150528, 157852, 196745, 151552, 158861, 174144, 152576, 192650, 197792, 202752, 184320, 175189, 178752, 193694, 190592, 179776, 147479, 191645, 203776, 185379, 186458, 148488, 198656, 187483, 194560, 180224, 199713, 141312, 182272, 200704, 195615, 183296, 201753, 142370, 181248, 161797, 153624, 162831, 154635, 0, 0, 0, 0, 0, 0, 0, 0),
    (133184, 134208, 131136, 132160, 135232, 136256, 137280, 138304, 168128, 145472, 169152, 146514, 7, 163968, 143424, 157696, 164992, 144464, 6, 147584, 169984, 139328, 158733, 171008, 140371, 148612, 166080, 141384, 159744, 167104, 142417, 5, 151552, 200832, 180800, 160782, 192640, 153600, 152586, 201856, 176674, 155776, 193664, 154654, 11, 156800, 202880, 177676, 22, 149632, 203904, 181859, 150680, 198656, 196617, 161920, 199680, 197665, 32, 172032, 184320, 182848, 162959, 185344, 183898, 173081, 186900, 190464, 188416, 187931, 189468, 194560, 178176, 174080, 195615, 191517, 175125, 179223, 0, 0),
    (135168, 136192, 133120, 134144, 166080, 141312, 155776, 131072, 132096, 167104, 142353, 156800, 137216, 138245, 139264, 168128, 159884, 140292, 169152, 160914, 143360, 164046, 161792, 144390, 165056, 162832, 145408, 194639, 157824, 146439, 195648, 158879, 176704, 170189, 180352, 153600, 171219, 181400, 177728, 202816, 186902, 154635, 203840, 187939, 151552, 178267, 184832, 152586, 196800, 172032, 147456, 179287, 185882, 148480, 197824, 173064, 32, 174080, 198720, 200724, 149504, 199777, 182912, 175125, 183961, 150537, 201762, 192512, 188416, 189468, 190464, 193566, 191517, 0, 0, 0, 0, 0, 0, 0),
)


def attend(queries_t, window, thresholds, top, total, summed, back, head, own):
    scale = HD ** (-0.5) * 1.4426950408889634
    key_tile = window[back, head, 0]
    value_tile = window[back, head, 1]
    iota = lax.broadcasted_iota(jnp.int32, (TILE, TOK), 0)
    seen = []
    for half in range(2):
        mask = iota >= thresholds[pl.ds(back * 2 + half, 1), :]
        if own:
            mask = mask & (iota + half * TILE <= lax.broadcasted_iota(jnp.int32, (TILE, TOK), 1))
        seen.append(mask)
    spans = [slice(member * TOK, (member + 1) * TOK) for member in range(GROUP)]
    if not own:
        old_tops = [top[head, :, span] for span in spans]
        old_totals = [total[head, :, span] for span in spans]
    raw = [
        jnp.dot(key_tile, queries_t[head, :, span], preferred_element_type=jnp.float32)
        for span in spans
    ]
    tops, totals, factors, products = [], [], [], []
    for member in range(GROUP):
        scores = jnp.concatenate(
            [
                jnp.where(seen[half], raw[member][half * TILE : (half + 1) * TILE], NEG)
                for half in range(2)
            ],
            axis=0,
        )
        new_top = jnp.max(scores, axis=0, keepdims=True)
        if not own:
            new_top = jnp.maximum(old_tops[member], new_top)
        scaled_top = new_top * scale
        weights = jnp.exp2(scores * scale - scaled_top)
        weight_sum = jnp.sum(weights, axis=0, keepdims=True)
        products.append(
            lax.dot_general(
                value_tile,
                weights.astype(jnp.bfloat16),
                (((0,), (0,)), ((), ())),
                preferred_element_type=jnp.float32,
            )
        )
        if not own:
            factors.append(jnp.exp2(old_tops[member] * scale - scaled_top))
            weight_sum = old_totals[member] * factors[member] + weight_sum
        tops.append(new_top)
        totals.append(weight_sum)
    for member, span in enumerate(spans):
        top[head, :, span] = tops[member]
        total[head, :, span] = totals[member]
        if own:
            summed[head, :, span] = products[member]
        else:
            summed[head, :, span] = summed[head, :, span] * factors[member] + products[member]


def kernel(
    q_ref,
    k_ref,
    v_ref,
    start_ref,
    list_ref,
    count_ref,
    o_ref,
    window,
    queries_t,
    thresholds,
    top,
    total,
    summed,
    result,
    q_here,
    kv_here,
    swapped,
    o_here,
    in_sem,
    out_sem,
    swap_send,
    swap_recv,
    send_sem,
    recv_sem,
):
    seq = lax.axis_index("seq")
    core = lax.axis_index("head")
    devices = lax.axis_size("seq")
    place = lax.rem(seq, SIDE)
    row_first = seq - place
    neighbours = (
        row_first + lax.rem(place + 1, SIDE),
        row_first + lax.rem(place + SIDE - 1, SIDE),
        lax.rem(seq + SIDE, devices),
        lax.rem(seq + devices - SIDE, devices),
    )
    last = place == SIDE - 1
    none = place == 0
    shifts = (
        jnp.where(last, 1 - SIDE, 1),
        jnp.where(none, SIDE - 1, -1),
        SIDE,
        -SIDE,
    )

    row = seq // SIDE
    rows = devices // SIDE
    not_last = row < rows - 1
    not_first = row > 0

    barrier = pltpu.get_barrier_semaphore()
    for where, there in zip(neighbours, (None, None, not_last, not_first)):

        def greet(where=where):
            pl.semaphore_signal(barrier, inc=1, device_id=(where, core), device_id_type=MESH)

        if there is None:
            greet()
        else:
            pl.when(there)(greet)

    ins = []
    for part, (ref, here) in enumerate(
        ((k_ref, kv_here.at[0]), (v_ref, kv_here.at[1]), (q_ref, q_here))
    ):
        ins.append(pltpu.make_async_copy(ref, here, in_sem.at[part]))
    for copy in ins:
        copy.start()

    kind = jnp.where(
        row == rows - 1,
        5 * SIDE,
        jnp.where(row == rows - 2, 4 * SIDE, lax.rem(row, SIDE) * SIDE),
    )
    kind = kind + place
    steps = len(PLAN[0])
    words = []
    for n in range(steps):
        word = PLAN[0][n]
        for c in range(1, len(PLAN)):
            word = jnp.where(kind == c, PLAN[c][n], word)
        words.append(word)

    def word_of(turn, place_in_turn):
        word = words[place_in_turn]
        for i in range(1, steps // TURN):
            word = jnp.where(turn == i, words[i * TURN + place_in_turn], word)
        return word

    tile_row = lax.broadcasted_iota(jnp.int32, (24, 1), 0)
    back_of = tile_row // 2
    half_of = tile_row - 2 * back_of
    tile_id = 2 * (seq - back_of) + half_of
    slots = list_ref.shape[1]
    listed = (list_ref[...] == tile_id) & (
        lax.broadcasted_iota(jnp.int32, (1, slots), 1) < count_ref[0]
    )
    live = jnp.max(jnp.where(listed, 1.0, 0.0), axis=1, keepdims=True)
    low = start_ref[...] - seq * TOK + (back_of * TOK - half_of * TILE)
    thresholds[...] = jnp.where(live > 0.5, low, FAR)
    for part in range(2):
        ins[part].wait()
        for mine in range(2):

            @pl.when(core == mine)
            def _():
                for head in range(HEADS):
                    window[0, head, part, mine * TILE : (mine + 1) * TILE, :] = kv_here[
                        part, :, mine * HEADS + head, :
                    ]
                    swapped[part, head] = kv_here[part, :, (1 - mine) * HEADS + head, :]

    pl.semaphore_signal(barrier, inc=1, device_id=(seq, 1 - core), device_id_type=MESH)
    pl.semaphore_wait(
        barrier, 3 + jnp.where(not_last, 1, 0) + jnp.where(not_first, 1, 0)
    )
    swaps = []
    for part in range(2):
        swaps.append(
            pltpu.make_async_remote_copy(
                src_ref=swapped.at[part],
                dst_ref=window.at[0, :, part, pl.ds(core * TILE, TILE), :],
                send_sem=swap_send.at[part],
                recv_sem=swap_recv.at[part],
                device_id=(seq, 1 - core),
                device_id_type=MESH,
            )
        )
    for copy in swaps:
        copy.start()

    ins[2].wait()
    for head in range(HEADS):
        for member in range(GROUP):
            queries_t[head, :, member * TOK : (member + 1) * TOK] = q_here[
                :, head * GROUP + member, :
            ].T

    def hand_on(n, back, head, part, direction):
        there = back + shifts[direction]
        return pltpu.make_async_remote_copy(
            src_ref=window.at[back, head, part],
            dst_ref=window.at[there, head, part],
            send_sem=send_sem.at[n, direction],
            recv_sem=recv_sem.at[there * HEADS + head, part],
            device_id=(neighbours[direction], core),
            device_id_type=MESH,
        )

    def wait_for(n, back, head, part, direction):
        return pltpu.make_async_remote_copy(
            src_ref=window.at[back, head, part],
            dst_ref=window.at[back, head, part],
            send_sem=send_sem.at[n, direction],
            recv_sem=recv_sem.at[back * HEADS + head, part],
            device_id=(neighbours[0], core),
            device_id_type=MESH,
        )

    def relay(n, code):
        slot = lax.rem(code // 32, 64)
        part = lax.rem(code // 16, 2)
        directions = lax.rem(code, 16)
        back, head = slot // HEADS, lax.rem(slot, HEADS)

        @pl.when((code >= 2048) & (back <= seq))
        def _():
            @pl.when(slot >= HEADS)
            def _():
                wait_for(n, back, head, part, 0).wait_recv()

            for direction in range(4):

                @pl.when(lax.rem(directions // (1 << direction), 2) == 1)
                def _():
                    hand_on(n, back, head, part, direction).start()

    def sent(n, code):
        slot = lax.rem(code // 32, 64)
        part = lax.rem(code // 16, 2)
        directions = lax.rem(code, 16)
        back, head = slot // HEADS, lax.rem(slot, HEADS)

        @pl.when((directions > 0) & (back <= seq))
        def _():
            for direction in range(4):

                @pl.when(lax.rem(directions // (1 << direction), 2) == 1)
                def _():
                    wait_for(n, back, head, part, direction).wait_send()

    for copy in swaps:
        copy.wait()

    for n in range(FIRST):
        relay(n, words[n] // 64)
    for head in range(HEADS):
        attend(queries_t, window, thresholds, top, total, summed, 0, head, True)

    def step(turn, _):
        for place_in_turn in range(TURN):
            n = turn * TURN + place_in_turn
            word = word_of(turn, place_in_turn)

            @pl.when(n >= FIRST)
            def _():
                relay(n, word // 64)

            slot = lax.rem(word, 64)

            @pl.when((slot >= HEADS) & (slot // HEADS <= seq))
            def _():
                back, head = slot // HEADS, lax.rem(slot, HEADS)
                attend(queries_t, window, thresholds, top, total, summed, back, head, False)

            @pl.when(turn >= LAG)
            def _():
                sent(n - LAG * TURN, word_of(turn - LAG, place_in_turn) // 64)

        return 0

    lax.fori_loop(0, steps // TURN, step, 0)

    outs = []
    for half in range(2):
        rows_out = slice(half * 128, (half + 1) * 128)
        for head in range(HEADS):
            for member in range(GROUP):
                span = slice(member * TOK + half * 128, member * TOK + (half + 1) * 128)
                inverse = 1.0 / total[head, :, span]
                result[rows_out, head * GROUP + member, :] = (summed[head, :, span] * inverse).T
        o_here[rows_out] = result[rows_out].astype(jnp.bfloat16)
        outs.append(
            pltpu.make_async_copy(o_here.at[rows_out], o_ref.at[rows_out], out_sem.at[half])
        )
        if half > 0:
            outs[half - 1].start()
    outs[-1].start()

    def finish(turn, _):
        for place_in_turn in range(TURN):
            sent(turn * TURN + place_in_turn, word_of(turn, place_in_turn) // 64)
        return 0

    lax.fori_loop(steps // TURN - LAG, steps // TURN, finish, 0)
    for copy in outs:
        copy.wait()


def body(queries, keys, values, doc_start, tile_list, tile_count):
    vmem = pl.BlockSpec(memory_space=pltpu.VMEM)
    hbm = pl.BlockSpec(memory_space=pltpu.HBM)
    lanes = GROUP * TOK
    return pl.pallas_call(
        kernel,
        out_shape=jax.ShapeDtypeStruct(queries.shape, jnp.bfloat16),
        in_specs=[hbm, hbm, hbm, vmem, vmem, pl.BlockSpec(memory_space=pltpu.SMEM)],
        out_specs=hbm,
        scratch_shapes=[
            pltpu.VMEM((BACK, HEADS, 2, TOK, HD), jnp.bfloat16),
            pltpu.VMEM((HEADS, HD, lanes), jnp.bfloat16),
            pltpu.VMEM((24, TOK), jnp.int32),
            pltpu.VMEM((HEADS, 1, lanes), jnp.float32),
            pltpu.VMEM((HEADS, 1, lanes), jnp.float32),
            pltpu.VMEM((HEADS, HD, lanes), jnp.float32),
            pltpu.VMEM(queries.shape, jnp.float32),
            pltpu.VMEM(queries.shape, jnp.bfloat16),
            pltpu.VMEM((2, TILE, 2 * HEADS, HD), jnp.bfloat16),
            pltpu.VMEM((2, HEADS, TILE, HD), jnp.bfloat16),
            pltpu.VMEM(queries.shape, jnp.bfloat16),
            pltpu.SemaphoreType.DMA((3,)),
            pltpu.SemaphoreType.DMA((2,)),
            pltpu.SemaphoreType.DMA((2,)),
            pltpu.SemaphoreType.DMA((2,)),
            pltpu.SemaphoreType.DMA((len(PLAN[0]), 4)),
            pltpu.SemaphoreType.DMA((ENTRIES, 2)),
        ],
        compiler_params=pltpu.CompilerParams(collective_id=0, has_side_effects=True),
    )(queries, keys, values, doc_start.reshape(1, TOK), tile_list, tile_count)


def solution(mesh):
    in_specs = (
        P("seq", "head", None),
        P(("seq", "head"), None, None),
        P(("seq", "head"), None, None),
        P("seq"),
        P("seq", None),
        P("seq"),
    )
    return jax.shard_map(
        body, mesh=mesh, in_specs=in_specs, out_specs=P("seq", "head", None), check_vma=False
    )
```

```python
import jax
import jax.numpy as jnp
from jax import lax
from jax.experimental import pallas as pl
from jax.experimental.pallas import tpu as pltpu
from jax.sharding import PartitionSpec as P

TILE = 128
REACH = 8
BACK = REACH + 1
SIDE = 4
HEADS = 4
GROUP = 4
TOK = 256
HD = 128
ENTRIES = BACK * HEADS
FIRST = 2
TURN = 10
LAG = 2
NEG = -1e30
FAR = 1 << 20
MESH = pl.DeviceIdType.MESH

PLAN = (
    (133376, 134400, 137664, 138688, 131264, 132288, 166336, 167377, 135360, 136384, 170368, 162048, 143680, 171411, 163087, 144704, 198662, 157952, 145472, 199713, 158989, 202752, 146503, 160128, 194624, 139264, 151680, 176256, 140292, 161152, 203790, 141411, 152704, 195658, 142431, 177280, 180741, 178176, 190528, 181782, 179224, 147456, 191552, 149527, 153885, 192576, 188928, 172032, 193600, 148480, 189982, 164168, 150556, 186368, 154889, 155648, 168203, 173076, 184320, 156672, 196608, 165196, 182288, 187392, 174107, 169234, 175104, 200725, 183321, 197632, 185376, 26, 201762, 0, 0, 0, 0, 0, 0, 0),
    (137536, 138560, 133440, 134464, 135424, 136448, 170112, 131392, 132416, 171155, 145408, 166080, 146439, 155904, 167121, 139328, 156940, 168128, 140356, 159872, 169170, 174592, 160910, 164096, 175637, 161792, 165136, 143616, 162831, 141376, 188608, 144646, 142400, 189632, 158080, 151557, 28, 196736, 147712, 152586, 197760, 159136, 153869, 176320, 192640, 154891, 190592, 148744, 202752, 177344, 184342, 149824, 191616, 193693, 203806, 180224, 185344, 150883, 26, 186432, 194560, 198665, 181248, 178200, 199713, 187456, 195584, 200731, 31, 182272, 179200, 201751, 34, 183296, 172057, 173076, 0, 0, 0, 0),
    (131392, 132416, 135488, 136512, 137472, 138496, 145472, 164032, 146503, 133440, 134464, 165072, 141312, 168320, 142341, 160000, 169362, 139584, 161038, 170432, 140612, 161792, 171475, 174144, 162831, 166336, 175189, 155776, 167377, 147456, 200832, 176128, 156812, 192640, 148488, 182272, 201890, 177152, 183318, 193689, 149504, 151582, 202880, 196608, 152586, 172032, 150537, 187008, 203939, 197632, 188448, 173076, 184320, 188059, 198656, 180224, 153600, 185370, 199680, 178209, 157952, 154635, 189468, 158976, 181261, 24, 194560, 143360, 190464, 179223, 195615, 144390, 191517, 0, 0, 0, 0, 0, 0, 0),
    (135424, 136448, 137472, 138496, 139264, 168128, 140292, 131328, 132352, 133376, 134400, 169170, 143360, 161792, 170432, 144390, 162831, 171456, 153875, 155904, 172032, 164288, 156940, 154891, 165312, 191120, 141312, 166208, 192157, 142341, 167232, 160145, 173056, 157696, 202836, 161166, 147712, 203840, 158720, 194723, 178765, 196800, 195743, 148736, 188616, 184832, 145408, 179799, 186496, 176128, 182784, 197856, 200704, 146439, 174080, 189632, 185884, 151680, 183834, 198720, 177177, 175104, 187542, 201749, 149504, 199771, 34, 152704, 192545, 150538, 193545, 180254, 181272, 0, 0, 0, 0, 0, 0, 0),
    (133376, 134400, 137664, 138688, 131264, 132288, 166336, 167377, 135360, 136384, 170368, 162048, 143680, 171411, 163087, 144704, 198662, 157952, 199713, 145472, 158989, 202752, 146503, 160128, 194624, 139264, 151680, 176256, 140292, 161152, 203790, 141411, 152704, 195658, 142400, 180767, 177285, 178176, 149504, 190550, 179223, 181760, 191576, 153856, 147456, 150528, 192605, 164169, 188928, 193630, 154891, 189952, 148508, 172032, 184328, 186368, 165200, 155648, 168192, 173076, 156672, 169216, 196620, 174098, 182272, 187419, 175104, 185365, 200730, 183321, 197664, 201762, 0, 0, 0, 0, 0, 0, 0, 0),
    (137536, 138560, 133440, 134464, 170112, 135424, 136448, 171155, 131392, 132416, 145408, 166080, 155904, 146432, 167111, 156945, 139328, 168140, 159872, 140352, 169156, 18, 160896, 174592, 164110, 161792, 175616, 165141, 16, 162816, 143616, 188623, 158080, 141376, 144640, 189638, 28, 159104, 142400, 151552, 196749, 147717, 152576, 197770, 192640, 153856, 176352, 148744, 154880, 177355, 184342, 202752, 190592, 193694, 149824, 180224, 185370, 203776, 191651, 194589, 150848, 186441, 178176, 198656, 187483, 195615, 199680, 181281, 179224, 200704, 182295, 172032, 183321, 201762, 173076, 0, 0, 0, 0, 0),
    (131392, 132416, 135488, 136512, 137472, 138496, 164032, 145472, 165056, 146512, 133440, 134471, 168320, 141312, 160000, 169362, 142341, 161024, 170446, 139584, 171456, 161811, 140612, 166336, 162816, 174159, 167377, 175168, 155797, 200832, 147456, 156812, 192640, 176128, 182272, 201890, 148480, 183304, 172057, 177152, 151574, 193664, 196638, 152586, 202880, 149504, 178176, 173076, 197632, 187040, 203939, 150528, 180233, 198656, 184320, 188059, 199713, 185344, 153600, 188442, 157952, 181272, 154635, 179223, 158989, 189468, 194560, 143360, 190464, 195615, 144390, 191517, 0, 0, 0, 0, 0, 0, 0, 0),
    (135424, 136448, 137472, 138496, 139264, 168128, 140288, 169156, 131328, 132352, 133376, 134418, 143360, 170432, 161792, 144390, 171456, 162835, 172047, 164288, 155904, 153856, 165328, 156940, 173056, 166208, 191124, 154891, 167232, 192145, 141341, 202816, 160128, 142341, 157696, 203840, 161187, 178752, 186496, 158720, 194702, 13, 147712, 188608, 195743, 179799, 196800, 184832, 145408, 148744, 189632, 176156, 174080, 187547, 200704, 146439, 182784, 197824, 185888, 151680, 175130, 198720, 177173, 183808, 199766, 201728, 149529, 192545, 152738, 193546, 150558, 180233, 181272, 0, 0, 0, 0, 0, 0, 0),
    (133376, 134400, 137664, 138688, 131264, 132288, 166336, 167377, 135360, 136384, 170368, 162048, 143680, 171411, 163087, 144704, 198662, 157952, 199713, 145472, 158989, 202752, 146503, 160128, 194624, 139264, 151680, 176256, 140292, 161152, 203790, 141411, 152704, 195658, 142400, 180767, 177285, 178176, 149504, 190550, 179223, 181760, 191576, 147456, 153856, 150528, 192605, 9, 172032, 188928, 193630, 164160, 189952, 148508, 8, 186368, 154880, 184331, 196608, 173056, 155668, 168192, 187419, 165184, 156672, 182288, 174092, 169216, 197650, 175104, 185376, 200725, 183322, 201753, 34, 0, 0, 0, 0, 0),
    (137536, 138560, 133440, 134464, 170112, 135424, 136448, 171155, 131392, 132416, 145408, 166080, 155904, 146432, 167111, 156945, 139328, 168140, 159872, 140352, 169156, 18, 160896, 174592, 164110, 161792, 175616, 165141, 16, 162816, 143616, 188623, 158080, 141376, 144640, 189638, 28, 159104, 142400, 151552, 196749, 147717, 152576, 197770, 192640, 153856, 176352, 148744, 154880, 190603, 184320, 202752, 177366, 193694, 149824, 191645, 185370, 203776, 180259, 194560, 150848, 186441, 195615, 198656, 181272, 178176, 199680, 187489, 27, 179200, 200704, 182295, 201728, 183330, 25, 172032, 173076, 0, 0, 0),
    (131392, 132416, 135488, 136512, 137472, 138496, 164032, 145472, 165056, 146512, 133440, 134471, 168320, 141312, 160000, 169362, 142341, 161024, 170446, 139584, 171456, 161811, 140612, 166336, 162816, 174159, 167377, 175168, 155797, 200832, 147456, 156812, 192640, 176128, 182272, 201890, 148480, 183304, 193689, 177152, 151582, 202880, 196630, 152586, 172032, 149504, 188416, 203939, 197632, 187040, 173076, 150528, 180233, 198656, 184320, 188059, 199713, 185344, 153600, 178202, 157952, 189468, 154635, 181272, 158989, 143360, 190464, 194560, 179223, 195615, 144390, 191517, 0, 0, 0, 0, 0, 0, 0, 0),
    (135424, 136448, 137472, 138496, 139264, 168128, 140288, 169156, 131328, 132352, 133376, 134418, 143360, 170432, 161792, 144390, 171456, 162835, 172047, 164288, 155904, 153856, 165328, 156940, 173056, 166208, 191124, 154891, 167232, 192145, 141341, 202816, 160128, 142341, 157696, 203840, 161187, 178766, 196800, 158720, 194701, 147712, 188608, 195743, 179799, 186496, 184832, 145408, 148744, 197824, 176160, 174080, 189660, 200704, 146432, 182791, 198720, 185882, 151680, 175104, 187541, 177179, 183808, 199744, 201750, 149529, 192545, 152738, 193546, 150528, 180254, 9, 181272, 0, 0, 0, 0, 0, 0, 0),
    (133376, 134400, 137664, 138688, 131264, 132288, 166336, 167377, 135360, 136384, 170368, 162048, 143680, 171411, 163087, 144704, 198662, 157952, 199713, 145472, 158989, 202752, 146503, 160128, 194624, 139264, 151680, 176256, 140292, 161152, 203790, 141411, 152704, 195658, 142400, 180767, 177285, 178176, 149504, 190550, 179223, 181760, 191576, 153856, 150557, 192585, 172032, 188928, 193630, 164160, 147456, 189980, 186368, 154891, 148480, 184328, 173076, 168192, 196608, 165200, 155648, 182272, 174080, 187419, 156672, 169228, 175104, 185344, 200722, 21, 183296, 197658, 25, 201760, 34, 0, 0, 0, 0, 0),
    (137536, 138560, 133440, 134464, 170112, 135424, 136448, 171155, 131392, 132416, 145408, 166080, 155904, 146432, 167111, 156945, 139328, 168140, 159872, 140352, 169156, 18, 160896, 174592, 164110, 161792, 175616, 165141, 16, 162816, 143616, 188623, 158080, 144640, 189638, 28, 159104, 141376, 151552, 196749, 147712, 142400, 152576, 197765, 10, 192640, 153856, 176352, 148744, 154880, 190603, 184320, 202752, 177366, 193694, 149824, 191645, 185370, 203776, 180259, 194560, 150848, 186441, 195615, 198656, 181272, 178176, 199680, 187489, 27, 179200, 200704, 182295, 201728, 183330, 25, 172032, 173076, 0, 0),
    (131392, 132416, 135488, 136512, 137472, 138496, 164032, 145472, 165056, 146512, 133440, 134471, 168320, 141312, 160000, 169362, 142341, 161024, 170446, 139584, 171456, 161811, 140612, 166336, 162816, 174159, 167377, 175168, 155797, 200832, 147456, 156812, 192640, 176128, 182272, 201890, 148480, 183304, 193689, 177152, 151582, 202880, 196630, 152586, 172032, 197632, 188448, 203939, 149504, 187008, 173076, 150528, 180233, 198656, 184320, 188059, 199713, 185344, 178202, 153600, 157952, 189468, 181272, 158989, 154624, 179211, 190464, 194583, 143360, 195615, 144390, 191517, 0, 0, 0, 0, 0, 0, 0, 0),
    (135424, 136448, 137472, 138496, 139264, 168128, 140288, 169156, 131328, 132352, 133376, 134418, 143360, 170432, 161792, 144390, 171456, 162835, 172047, 164288, 155904, 153856, 165328, 156940, 173056, 166208, 191124, 154891, 167232, 192145, 141341, 202816, 160128, 142341, 203840, 161187, 178752, 157710, 196800, 194688, 147712, 158733, 188608, 195743, 179776, 186496, 184855, 148744, 197824, 176160, 174080, 189660, 200704, 145408, 182784, 198720, 185882, 175125, 187520, 177152, 151707, 183830, 199744, 201728, 146457, 192512, 149537, 34, 193536, 152711, 30, 180224, 150538, 9, 181272, 0, 0, 0, 0, 0),
    (131328, 132352, 137344, 138368, 135488, 136512, 166336, 167377, 170368, 133568, 134592, 162048, 143680, 171411, 163087, 144704, 198662, 157952, 199680, 145505, 158989, 202752, 146503, 160128, 194624, 139264, 151680, 176256, 140292, 161152, 203790, 141411, 152704, 195658, 142400, 180767, 177285, 178176, 149504, 190550, 179223, 181760, 191576, 172032, 150557, 192585, 164160, 188928, 193630, 153856, 147456, 184320, 154891, 186368, 189952, 148508, 173056, 196616, 168212, 165184, 187392, 155648, 182288, 174107, 169234, 197632, 175136, 185344, 200725, 156672, 183322, 201740, 25, 34, 0, 0, 0, 0, 0, 0),
    (131392, 132416, 137472, 138496, 135424, 136448, 170112, 171155, 133440, 134464, 166080, 143424, 155904, 167121, 144454, 156928, 168128, 174604, 159872, 169170, 175637, 160896, 164096, 141582, 161792, 165136, 142597, 162816, 188608, 151567, 158080, 189660, 152586, 159104, 196736, 153869, 192640, 197760, 154912, 11, 147712, 176320, 202752, 184320, 190592, 149824, 178176, 177344, 203798, 35, 193664, 191616, 150878, 29, 148736, 180224, 198656, 145417, 185344, 186432, 199688, 146458, 139264, 181248, 200737, 7, 179200, 187456, 172056, 194560, 182272, 201751, 27, 195584, 183330, 173087, 140313, 20, 4, 0),
    (135424, 136448, 131392, 132416, 137536, 138560, 133440, 134464, 164032, 139328, 165056, 140368, 4, 168320, 160000, 169362, 161038, 170432, 141312, 161792, 171475, 142341, 182272, 166336, 174144, 162831, 167377, 151872, 183296, 200857, 175189, 155776, 192640, 152906, 187008, 201890, 176128, 156812, 193664, 147678, 177152, 188032, 202902, 196635, 172032, 143360, 188416, 197664, 203939, 180224, 184320, 144384, 173062, 178196, 157952, 198656, 148672, 189448, 28, 185344, 199680, 145690, 159009, 181261, 149528, 146695, 194560, 150528, 179209, 23, 153600, 190464, 195584, 154655, 11, 191517, 0, 0, 0, 0),
    (133376, 134400, 135424, 136448, 168128, 131328, 132352, 162048, 169170, 163087, 137472, 138496, 170432, 139264, 191104, 171456, 140307, 4, 192128, 145664, 164317, 194688, 146695, 165328, 157696, 141312, 166208, 158733, 142336, 167237, 195712, 172032, 202833, 31, 147456, 203875, 184832, 173076, 196800, 143360, 176128, 148488, 188608, 200704, 178752, 186496, 144384, 185862, 179776, 197850, 153728, 177152, 174103, 189664, 154752, 201728, 182784, 198742, 151580, 175104, 187531, 160034, 199744, 152597, 183808, 192539, 33, 161024, 193546, 25, 155648, 180224, 149518, 156702, 181248, 150540, 24, 9, 0, 0),
    (131200, 132224, 135360, 136384, 163904, 137408, 138432, 164944, 133248, 134272, 168000, 155776, 141376, 169042, 156812, 142400, 198661, 161920, 199680, 143457, 162959, 202752, 144454, 159872, 165888, 139264, 147584, 166929, 140292, 160896, 194638, 170048, 148616, 176256, 171091, 157824, 203811, 151552, 158861, 195648, 145439, 180736, 177302, 146439, 181760, 190552, 152576, 149514, 191552, 178205, 188928, 192576, 179223, 150537, 193600, 153694, 184320, 196608, 172032, 189980, 186368, 154699, 185370, 187392, 173083, 182272, 200724, 174080, 183321, 197632, 175136, 21, 201762, 0, 0, 0, 0, 0, 0, 0),
    (137280, 138304, 135232, 136256, 131136, 132160, 163968, 143360, 133184, 134208, 165008, 144390, 170112, 172096, 159744, 171155, 145472, 160782, 168128, 146503, 155776, 169170, 173120, 156820, 166028, 176128, 139264, 167057, 149504, 188608, 177152, 140310, 189636, 150528, 157852, 196745, 151552, 158861, 174144, 152576, 192650, 197792, 202752, 184320, 175189, 178752, 193694, 190592, 179776, 147479, 191645, 203776, 185379, 186458, 148488, 198656, 187483, 194560, 180224, 199713, 141312, 182272, 200704, 195615, 183296, 201753, 142370, 181248, 161797, 153624, 162831, 154635, 0, 0, 0, 0, 0, 0, 0, 0),
    (133184, 134208, 131136, 132160, 135232, 136256, 137280, 138304, 168128, 145472, 169152, 146514, 7, 163968, 143424, 157696, 164992, 144464, 6, 147584, 169984, 139328, 158733, 171008, 140371, 148612, 166080, 141384, 159744, 167104, 142417, 5, 151552, 200832, 180800, 160782, 192640, 153600, 152586, 201856, 176674, 155776, 193664, 154654, 11, 156800, 202880, 177676, 22, 149632, 203904, 181859, 150680, 198656, 196617, 161920, 199680, 197665, 32, 172032, 184320, 182848, 162959, 185344, 183898, 173081, 186900, 190464, 188416, 187931, 189468, 194560, 178176, 174080, 195615, 191517, 175125, 179223, 0, 0),
    (135168, 136192, 133120, 134144, 166080, 141312, 155776, 131072, 132096, 167104, 142353, 156800, 137216, 138245, 139264, 168128, 159884, 140292, 169152, 160914, 143360, 164046, 161792, 144390, 165056, 162832, 145408, 194639, 157824, 146439, 195648, 158879, 176704, 170189, 180352, 153600, 171219, 181400, 177728, 202816, 186902, 154635, 203840, 187939, 151552, 178267, 184832, 152586, 196800, 172032, 147456, 179287, 185882, 148480, 197824, 173064, 32, 174080, 198720, 200724, 149504, 199777, 182912, 175125, 183961, 150537, 201762, 192512, 188416, 189468, 190464, 193566, 191517, 0, 0, 0, 0, 0, 0, 0),
)


def attend(queries_t, window, thresholds, top, total, summed, back, head, own):
    scale = HD ** (-0.5) * 1.4426950408889634
    key_tile = window[back, head, 0]
    value_tile = window[back, head, 1]
    iota = lax.broadcasted_iota(jnp.int32, (TILE, TOK), 0)
    seen = []
    for half in range(2):
        mask = iota >= thresholds[pl.ds(back * 2 + half, 1), :]
        if own:
            mask = mask & (iota + half * TILE <= lax.broadcasted_iota(jnp.int32, (TILE, TOK), 1))
        seen.append(mask)
    spans = [slice(member * TOK, (member + 1) * TOK) for member in range(GROUP)]
    if not own:
        old_tops = [top[head, :, span] for span in spans]
        old_totals = [total[head, :, span] for span in spans]
    raw = [
        jnp.dot(key_tile, queries_t[head, :, span], preferred_element_type=jnp.float32)
        for span in spans
    ]
    tops, totals, factors, products = [], [], [], []
    for member in range(GROUP):
        scores = jnp.concatenate(
            [
                jnp.where(seen[half], raw[member][half * TILE : (half + 1) * TILE], NEG)
                for half in range(2)
            ],
            axis=0,
        )
        new_top = jnp.max(scores, axis=0, keepdims=True)
        if not own:
            new_top = jnp.maximum(old_tops[member], new_top)
        scaled_top = new_top * scale
        weights = jnp.exp2(scores * scale - scaled_top)
        weight_sum = jnp.sum(weights, axis=0, keepdims=True)
        products.append(
            lax.dot_general(
                value_tile,
                weights.astype(jnp.bfloat16),
                (((0,), (0,)), ((), ())),
                preferred_element_type=jnp.float32,
            )
        )
        if not own:
            factors.append(jnp.exp2(old_tops[member] * scale - scaled_top))
            weight_sum = old_totals[member] * factors[member] + weight_sum
        tops.append(new_top)
        totals.append(weight_sum)
    for member, span in enumerate(spans):
        top[head, :, span] = tops[member]
        total[head, :, span] = totals[member]
        if own:
            summed[head, :, span] = products[member]
        else:
            summed[head, :, span] = summed[head, :, span] * factors[member] + products[member]


def kernel(
    q_ref,
    k_ref,
    v_ref,
    start_ref,
    list_ref,
    count_ref,
    o_ref,
    window,
    queries_t,
    thresholds,
    top,
    total,
    summed,
    result,
    q_here,
    kv_here,
    swapped,
    in_sem,
    swap_send,
    swap_recv,
    send_sem,
    recv_sem,
):
    seq = lax.axis_index("seq")
    core = lax.axis_index("head")
    devices = lax.axis_size("seq")
    place = lax.rem(seq, SIDE)
    row_first = seq - place
    neighbours = (
        row_first + lax.rem(place + 1, SIDE),
        row_first + lax.rem(place + SIDE - 1, SIDE),
        lax.rem(seq + SIDE, devices),
        lax.rem(seq + devices - SIDE, devices),
    )
    last = place == SIDE - 1
    none = place == 0
    shifts = (
        jnp.where(last, 1 - SIDE, 1),
        jnp.where(none, SIDE - 1, -1),
        SIDE,
        -SIDE,
    )

    row = seq // SIDE
    rows = devices // SIDE
    not_last = row < rows - 1
    not_first = row > 0

    barrier = pltpu.get_barrier_semaphore()
    for where, there in zip(neighbours, (None, None, not_last, not_first)):

        def greet(where=where):
            pl.semaphore_signal(barrier, inc=1, device_id=(where, core), device_id_type=MESH)

        if there is None:
            greet()
        else:
            pl.when(there)(greet)

    ins = []
    for part, (ref, here) in enumerate(
        ((k_ref, kv_here.at[0]), (v_ref, kv_here.at[1]), (q_ref, q_here))
    ):
        ins.append(pltpu.make_async_copy(ref, here, in_sem.at[part]))
    for copy in ins:
        copy.start()

    kind = jnp.where(
        row == rows - 1,
        5 * SIDE,
        jnp.where(row == rows - 2, 4 * SIDE, lax.rem(row, SIDE) * SIDE),
    )
    kind = kind + place
    steps = len(PLAN[0])
    words = []
    for n in range(steps):
        word = PLAN[0][n]
        for c in range(1, len(PLAN)):
            word = jnp.where(kind == c, PLAN[c][n], word)
        words.append(word)

    def word_of(turn, place_in_turn):
        word = words[place_in_turn]
        for i in range(1, steps // TURN):
            word = jnp.where(turn == i, words[i * TURN + place_in_turn], word)
        return word

    tile_row = lax.broadcasted_iota(jnp.int32, (24, 1), 0)
    back_of = tile_row // 2
    half_of = tile_row - 2 * back_of
    tile_id = 2 * (seq - back_of) + half_of
    slots = list_ref.shape[1]
    listed = (list_ref[...] == tile_id) & (
        lax.broadcasted_iota(jnp.int32, (1, slots), 1) < count_ref[0]
    )
    live = jnp.max(jnp.where(listed, 1.0, 0.0), axis=1, keepdims=True)
    low = start_ref[...] - seq * TOK + (back_of * TOK - half_of * TILE)
    thresholds[...] = jnp.where(live > 0.5, low, FAR)
    for part in range(2):
        ins[part].wait()
        for mine in range(2):

            @pl.when(core == mine)
            def _():
                for head in range(HEADS):
                    window[0, head, part, mine * TILE : (mine + 1) * TILE, :] = kv_here[
                        part, :, mine * HEADS + head, :
                    ]
                    swapped[part, head] = kv_here[part, :, (1 - mine) * HEADS + head, :]

    pl.semaphore_signal(barrier, inc=1, device_id=(seq, 1 - core), device_id_type=MESH)
    pl.semaphore_wait(
        barrier, 3 + jnp.where(not_last, 1, 0) + jnp.where(not_first, 1, 0)
    )
    swaps = []
    for part in range(2):
        swaps.append(
            pltpu.make_async_remote_copy(
                src_ref=swapped.at[part],
                dst_ref=window.at[0, :, part, pl.ds(core * TILE, TILE), :],
                send_sem=swap_send.at[part],
                recv_sem=swap_recv.at[part],
                device_id=(seq, 1 - core),
                device_id_type=MESH,
            )
        )
    for copy in swaps:
        copy.start()

    ins[2].wait()
    for head in range(HEADS):
        for member in range(GROUP):
            queries_t[head, :, member * TOK : (member + 1) * TOK] = q_here[
                :, head * GROUP + member, :
            ].T

    def hand_on(n, back, head, part, direction):
        there = back + shifts[direction]
        return pltpu.make_async_remote_copy(
            src_ref=window.at[back, head, part],
            dst_ref=window.at[there, head, part],
            send_sem=send_sem.at[n, direction],
            recv_sem=recv_sem.at[there * HEADS + head, part],
            device_id=(neighbours[direction], core),
            device_id_type=MESH,
        )

    def wait_for(n, back, head, part, direction):
        return pltpu.make_async_remote_copy(
            src_ref=window.at[back, head, part],
            dst_ref=window.at[back, head, part],
            send_sem=send_sem.at[n, direction],
            recv_sem=recv_sem.at[back * HEADS + head, part],
            device_id=(neighbours[0], core),
            device_id_type=MESH,
        )

    def relay(n, code):
        slot = lax.rem(code // 32, 64)
        part = lax.rem(code // 16, 2)
        directions = lax.rem(code, 16)
        back, head = slot // HEADS, lax.rem(slot, HEADS)

        @pl.when((code >= 2048) & (back <= seq))
        def _():
            @pl.when(slot >= HEADS)
            def _():
                wait_for(n, back, head, part, 0).wait_recv()

            for direction in range(4):

                @pl.when(lax.rem(directions // (1 << direction), 2) == 1)
                def _():
                    hand_on(n, back, head, part, direction).start()

    def sent(n, code):
        slot = lax.rem(code // 32, 64)
        part = lax.rem(code // 16, 2)
        directions = lax.rem(code, 16)
        back, head = slot // HEADS, lax.rem(slot, HEADS)

        @pl.when((directions > 0) & (back <= seq))
        def _():
            for direction in range(4):

                @pl.when(lax.rem(directions // (1 << direction), 2) == 1)
                def _():
                    wait_for(n, back, head, part, direction).wait_send()

    for copy in swaps:
        copy.wait()

    for n in range(FIRST):
        relay(n, words[n] // 64)
    for head in range(HEADS):
        attend(queries_t, window, thresholds, top, total, summed, 0, head, True)

    def step(turn, _):
        for place_in_turn in range(TURN):
            n = turn * TURN + place_in_turn
            word = word_of(turn, place_in_turn)

            @pl.when(n >= FIRST)
            def _():
                relay(n, word // 64)

            slot = lax.rem(word, 64)

            @pl.when((slot >= HEADS) & (slot // HEADS <= seq))
            def _():
                back, head = slot // HEADS, lax.rem(slot, HEADS)
                attend(queries_t, window, thresholds, top, total, summed, back, head, False)

            @pl.when(turn >= LAG)
            def _():
                sent(n - LAG * TURN, word_of(turn - LAG, place_in_turn) // 64)

        return 0

    lax.fori_loop(0, steps // TURN, step, 0)

    for half in range(2):
        rows_out = slice(half * 128, (half + 1) * 128)
        for head in range(HEADS):
            for member in range(GROUP):
                span = slice(member * TOK + half * 128, member * TOK + (half + 1) * 128)
                inverse = 1.0 / total[head, :, span]
                result[rows_out, head * GROUP + member, :] = (summed[head, :, span] * inverse).T
        o_ref[rows_out] = result[rows_out].astype(jnp.bfloat16)

    def finish(turn, _):
        for place_in_turn in range(TURN):
            sent(turn * TURN + place_in_turn, word_of(turn, place_in_turn) // 64)
        return 0

    lax.fori_loop(steps // TURN - LAG, steps // TURN, finish, 0)


def body(queries, keys, values, doc_start, tile_list, tile_count):
    vmem = pl.BlockSpec(memory_space=pltpu.VMEM)
    hbm = pl.BlockSpec(memory_space=pltpu.HBM)
    lanes = GROUP * TOK
    return pl.pallas_call(
        kernel,
        out_shape=jax.ShapeDtypeStruct(queries.shape, jnp.bfloat16),
        in_specs=[hbm, hbm, hbm, vmem, vmem, pl.BlockSpec(memory_space=pltpu.SMEM)],
        out_specs=vmem,
        scratch_shapes=[
            pltpu.VMEM((BACK, HEADS, 2, TOK, HD), jnp.bfloat16),
            pltpu.VMEM((HEADS, HD, lanes), jnp.bfloat16),
            pltpu.VMEM((24, TOK), jnp.int32),
            pltpu.VMEM((HEADS, 1, lanes), jnp.float32),
            pltpu.VMEM((HEADS, 1, lanes), jnp.float32),
            pltpu.VMEM((HEADS, HD, lanes), jnp.float32),
            pltpu.VMEM(queries.shape, jnp.float32),
            pltpu.VMEM(queries.shape, jnp.bfloat16),
            pltpu.VMEM((2, TILE, 2 * HEADS, HD), jnp.bfloat16),
            pltpu.VMEM((2, HEADS, TILE, HD), jnp.bfloat16),
            pltpu.SemaphoreType.DMA((3,)),
            pltpu.SemaphoreType.DMA((2,)),
            pltpu.SemaphoreType.DMA((2,)),
            pltpu.SemaphoreType.DMA((len(PLAN[0]), 4)),
            pltpu.SemaphoreType.DMA((ENTRIES, 2)),
        ],
        compiler_params=pltpu.CompilerParams(
            collective_id=0, has_side_effects=True, vmem_limit_bytes=32 * 1024 * 1024
        ),
    )(queries, keys, values, doc_start.reshape(1, TOK), tile_list, tile_count)


def solution(mesh):
    in_specs = (
        P("seq", "head", None),
        P(("seq", "head"), None, None),
        P(("seq", "head"), None, None),
        P("seq"),
        P("seq", None),
        P("seq"),
    )
    return jax.shard_map(
        body, mesh=mesh, in_specs=in_specs, out_specs=P("seq", "head", None), check_vma=False
    )
```
